16 devices in a mesh: rep: 1, dp: 16 (over x, y, z, core).
Axes of the slice: x: 2, y: 2, z: 2, core: 2. Of those that a mesh axis runs over, the one named last changes fastest.
Arguments:
- x: bfloat16 [16, 2048, 768], P(('rep', 'dp'))
- dy: bfloat16 [16, 2048, 768], P(('rep', 'dp'))
- wq: bfloat16 [2, 768, 768], P(None, 'dp')
- wk: bfloat16 [2, 768, 128], P(None, 'dp')
- wv: bfloat16 [2, 768, 128], P(None, 'dp')
- wo: bfloat16 [2, 768, 768], P(None, 'dp')
- w_gate: bfloat16 [2, 768, 2048], P(None, 'dp')
- w_up: bfloat16 [2, 768, 2048], P(None, 'dp')
- w_down: bfloat16 [2, 2048, 768], P(None, 'dp')
Outputs:
- output 1: bfloat16 [16, 2048, 768], P(('rep', 'dp'))
- output 2: bfloat16 [2, 768, 768], P('rep', 'dp')
- output 3: bfloat16 [2, 768, 128], P('rep', 'dp')
- output 4: bfloat16 [2, 768, 128], P('rep', 'dp')
- output 5: bfloat16 [2, 768, 768], P('rep', 'dp')
- output 6: bfloat16 [2, 768, 2048], P('rep', 'dp')
- output 7: bfloat16 [2, 768, 2048], P('rep', 'dp')
- output 8: bfloat16 [2, 2048, 768], P('rep', 'dp')
All inputs are finite; a program needn't handle non-finite values.
Results may differ from the reference program's by a relative error of at most 0.0285.
Values are sent between devices in bfloat16 or wider.
A program may use at most 2 GiB of HBM per device.

```python
import jax
import jax.numpy as jnp
from jax import lax

SEQUENCES = 16
TOKENS = 2048
D = 768
HEADS = 6
KV_HEADS = 1
HEAD = 128
FF = 2048
LAYERS = 2
THETA = 10000
NAMES = ("wq", "wk", "wv", "wo", "w_gate", "w_up", "w_down")
SHAPES = {
    "wq": (LAYERS, D, HEADS * HEAD),
    "wk": (LAYERS, D, KV_HEADS * HEAD),
    "wv": (LAYERS, D, KV_HEADS * HEAD),
    "wo": (LAYERS, HEADS * HEAD, D),
    "w_gate": (LAYERS, D, FF),
    "w_up": (LAYERS, D, FF),
    "w_down": (LAYERS, FF, D),
}


def bump(key, n, height):
    away = (jnp.arange(n, dtype=jnp.int32) - jax.random.randint(key, (), 0, n, jnp.int32)) % n
    return jnp.where(away < n // 8, height, 1.0)


def together(key, own, strength):
    shared = jax.random.normal(key, own.shape[1:], jnp.float32)
    return (own + strength * shared) * lax.rsqrt(1 + strength * strength)


def setup_inputs(seed: int = 0, part: int = 0) -> dict:
    kx, kdy, ka, kb, kz, kf, kh, kl, *keys = jax.random.split(jax.random.key(seed), 8 + 3 * len(NAMES))
    kx, kdy, ka, kb = (jax.random.fold_in(k, part) for k in (kx, kdy, ka, kb))
    kw, km, kv = (keys[i::3] for i in range(3))
    shape = (SEQUENCES, TOKENS, D)
    much_x, much_dy = jax.random.uniform(kz, (2,), jnp.float32, 0.0, 1.0)
    loud = 2.0 ** jax.random.uniform(jax.random.fold_in(kz, 1), (), jnp.float32, -1.0, 2.0)
    layers = 2.0 ** jax.random.uniform(kl, (LAYERS, 1, 1), jnp.float32, -1.0, 1.0)
    times = {"wq": 1.0, "wk": 1.0, "wv": 2.0, "wo": layers, "w_gate": 1.0, "w_up": bump(kh, FF, 4.0), "w_down": layers}
    x = together(ka, jax.random.normal(kx, shape, jnp.float32), much_x) * bump(kf, D, 4.0)
    dy = together(kb, jax.random.normal(kdy, shape, jnp.float32), much_dy)
    drawn = {"x": x.astype(jnp.bfloat16), "dy": (loud * dy * (SEQUENCES * TOKENS) ** -0.5).astype(jnp.bfloat16)}
    for key, name in zip(kw, NAMES, strict=True):
        drawn[name] = (jax.random.normal(key, SHAPES[name], jnp.float32) * SHAPES[name][1] ** -0.5 * times[name]).astype(jnp.bfloat16)
    return drawn


def matmul(a, w):
    return jnp.dot(a, w, preferred_element_type=jnp.float32).astype(jnp.bfloat16)


def normed(h):
    wide = h.astype(jnp.float32)
    scale = lax.rsqrt(jnp.mean(wide**2, -1, keepdims=True) + 1e-6)
    return (wide * scale).astype(jnp.bfloat16)


def turned(t, theta):
    half = t.shape[-1] // 2
    angle = jnp.arange(t.shape[0], dtype=jnp.float32)[:, None] * theta ** (-jnp.arange(half, dtype=jnp.float32) / half)
    cos, sin = jnp.cos(angle)[:, None], jnp.sin(angle)[:, None]
    a, b = t[..., :half].astype(jnp.float32), t[..., half:].astype(jnp.float32)
    return jnp.concatenate([a * cos - b * sin, b * cos + a * sin], -1).astype(jnp.bfloat16)


def seen_by(q, k, v):
    tokens, kv = q.shape[0], k.shape[1]
    q = q.reshape(tokens, kv, -1, q.shape[-1])
    scores = jnp.einsum("tgsd,ugd->gstu", q.astype(jnp.float32), k.astype(jnp.float32)) * q.shape[-1] ** -0.5
    place = jnp.arange(tokens)
    weights = jax.nn.softmax(jnp.where(place[:, None] >= place, scores, -jnp.inf), -1).astype(jnp.bfloat16)
    return jnp.einsum("gstu,ugd->tgsd", weights.astype(jnp.float32), v.astype(jnp.float32)).astype(jnp.bfloat16).reshape(tokens, -1)


def layer(h, w):
    a = normed(h)
    q, k = (turned(matmul(a, w[name]).reshape(h.shape[0], -1, HEAD), THETA) for name in ("wq", "wk"))
    h = h + matmul(seen_by(q, k, matmul(a, w["wv"]).reshape(h.shape[0], -1, HEAD)), w["wo"])
    b = normed(h)
    gate = jnp.dot(b, w["w_gate"], preferred_element_type=jnp.float32)
    up = jnp.dot(b, w["w_up"], preferred_element_type=jnp.float32)
    return h + matmul((jax.nn.silu(gate) * up).astype(jnp.bfloat16), w["w_down"])


def stack(weights, h):
    return lax.scan(lambda h, w: (layer(h, w), None), h, weights)[0]


def reference(x, dy, wq, wk, wv, wo, w_gate, w_up, w_down):
    weights = dict(zip(NAMES, (wq, wk, wv, wo, w_gate, w_up, w_down), strict=True))

    def take(so_far, sequence):
        h, by_y = sequence
        _, back = jax.vjp(stack, weights, h)
        by_weights, by_h = back(by_y)
        return jax.tree.map(lambda total, term: total + term.astype(jnp.float32), so_far, by_weights), by_h

    none_yet = {name: jnp.zeros(w.shape, jnp.float32) for name, w in weights.items()}
    by_weights, by_x = lax.scan(take, none_yet, (x, dy))
    return (by_x, *(by_weights[name].astype(jnp.bfloat16) for name in NAMES))
```

```python
import functools

import jax
import jax.numpy as jnp
import numpy as np
from jax import lax
from jax.experimental import pallas as pl
from jax.experimental.pallas import tpu as pltpu
from jax.sharding import PartitionSpec as P

HEAD = 128
THETA = 10000
EPS = 1e-6
NEG = -1e30
LOG2E = 1.4426950408889634
BF, F32 = jnp.bfloat16, jnp.float32
MIB = 2**20


def _dot(a, b, ca=1, cb=0):
    return lax.dot_general(a, b, (((ca,), (cb,)), ((), ())), preferred_element_type=F32)


def _scale(wide):
    return lax.rsqrt(jnp.mean(wide * wide, -1, keepdims=True) + EPS)


def _normed(h):
    wide = h.astype(F32)
    return (wide * _scale(wide)).astype(BF)


def _norm_back(h, da):
    wide = h.astype(F32)
    scale = _scale(wide)
    a = wide * scale
    return scale * (da - a * jnp.mean(a * da, -1, keepdims=True))


def _turn(t, cos, sin):
    return t * cos + pltpu.roll(t, t.shape[1] // 2, 1) * sin


def _whole(shape):
    return pl.BlockSpec(shape, lambda *_: (0,) * len(shape), pipeline_mode=pl.Buffered(1))


def _params(*kinds, vmem=60):
    return pltpu.CompilerParams(dimension_semantics=kinds, vmem_limit_bytes=vmem * MIB)


def _cost(flops, *arrays):
    return pl.CostEstimate(flops=flops, transcendentals=0, bytes_accessed=sum(a.size * a.dtype.itemsize for a in arrays))


def _like(*shape, dtype=BF):
    return jax.ShapeDtypeStruct(shape, dtype)


def rotary(tokens):
    half = HEAD // 2
    angle = np.arange(tokens, dtype=np.float32)[:, None] * (np.float32(THETA) ** (-np.arange(half, dtype=np.float32) / np.float32(half)))
    angle = angle.astype(np.float64)
    cos, sin = np.cos(angle), np.sin(angle)
    return np.concatenate([cos, cos], -1).astype(np.float32), np.concatenate([-sin, sin], -1).astype(np.float32)


def _qkv_kernel(h_ref, w_ref, cos_ref, sin_ref, q_ref, k_ref, v_ref):
    a = _normed(h_ref[...])
    cos, sin = cos_ref[...], sin_ref[...]
    d = q_ref.shape[1]
    for n in range(0, d + HEAD, 2 * HEAD):
        wide = min(2 * HEAD, w_ref.shape[1] - n)
        t = _dot(a, w_ref[:, n : n + wide]).astype(BF)
        for at in range(n, n + wide, HEAD):
            own = t[:, at - n : at - n + HEAD]
            if at < d:
                q_ref[:, at : at + HEAD] = _turn(own.astype(F32), cos, sin).astype(BF)
            elif at < d + HEAD:
                k_ref[...] = _turn(own.astype(F32), cos, sin).astype(BF)
            else:
                v_ref[...] = own


def qkv(h, w, cos, sin, bt=512):
    n, d = h.shape
    wide = w.shape[1] - 2 * HEAD
    rows = lambda c: pl.BlockSpec((bt, c), lambda i: (i, 0))
    return pl.pallas_call(
        _qkv_kernel,
        grid=(n // bt,),
        in_specs=[rows(d), _whole(w.shape), rows(HEAD), rows(HEAD)],
        out_specs=[rows(wide), rows(HEAD), rows(HEAD)],
        out_shape=[_like(n, wide), _like(n, HEAD), _like(n, HEAD)],
        compiler_params=_params("arbitrary"),
        cost_estimate=_cost(2 * n * d * w.shape[1], h, h, w, cos, sin),
        name="qkv",
    )(h, w, cos, sin)


def _below(keys, queries, first):
    gap = lax.broadcasted_iota(jnp.int32, (keys, queries), 1) - lax.broadcasted_iota(jnp.int32, (keys, queries), 0)
    return gap >= -first


def _attn_kernel(q_ref, k_ref, v_ref, wo_ref, h_ref, o_ref, lse_ref, h2_ref, top_s, mix_s, *, bk):
    bq, heads = q_ref.shape[0], q_ref.shape[1] // HEAD
    iq = pl.program_id(0)
    e = HEAD**-0.5 * LOG2E
    ones = jnp.ones((8, bk), BF)
    top_s[...] = jnp.full_like(top_s, NEG)
    mix_s[...] = jnp.zeros_like(mix_s)

    def block(start, at, masked):
        here = pl.ds(start, bk)
        k = k_ref[here, :]
        values = jnp.concatenate([v_ref[here, :].T, ones], axis=0)
        scores = [_dot(k, q_ref[at:, n * HEAD : (n + 1) * HEAD], 1, 1) for n in range(heads)]
        ok = _below(bk, bq - at, 0) if masked else None
        weights, keeps = [], []
        for n, s in enumerate(scores):
            if masked:
                s = jnp.where(ok, s, 2 * NEG)
            old = top_s[n : n + 1, at:]
            top = jnp.maximum(old, s.max(axis=0, keepdims=True))
            top_s[n : n + 1, at:] = top
            weights.append(jnp.exp2((s - top) * e).astype(BF))
            keeps.append(jnp.exp2((old - top) * e))
        for n, (p, keep) in enumerate(zip(weights, keeps)):
            mix_s[n, :, at:] = mix_s[n, :, at:] * keep + _dot(values, p)

    lax.fori_loop(0, iq * (bq // bk), lambda j, _: block(pl.multiple_of(j * bk, bk), 0, False), None)
    for at in range(0, bq, bk):
        block(pl.multiple_of(iq * bq + at, bk), at, True)
    outs = []
    for n in range(heads):
        total = mix_s[n, HEAD : HEAD + 1, :]
        outs.append((mix_s[n, :HEAD, :] * (1 / total)).T.astype(BF))
        lse_ref[n : n + 1, :] = top_s[n : n + 1, :] * e + jnp.log2(total)
    o = jnp.concatenate(outs, axis=1)
    o_ref[...] = o
    h2_ref[...] = (h_ref[...].astype(F32) + _dot(o, wo_ref[...]).astype(BF).astype(F32)).astype(BF)


def attn(q, k, v, wo, h, bq=512, bk=256):
    n, d = h.shape
    heads = q.shape[1] // HEAD
    rows = lambda c: pl.BlockSpec((bq, c), lambda i: (i, 0))
    return pl.pallas_call(
        functools.partial(_attn_kernel, bk=bk),
        grid=(n // bq,),
        in_specs=[rows(q.shape[1]), _whole(k.shape), _whole(v.shape), _whole(wo.shape), rows(d)],
        out_specs=[rows(q.shape[1]), pl.BlockSpec((heads, bq), lambda i: (0, i)), rows(d)],
        out_shape=[_like(*q.shape), _like(heads, n, dtype=F32), _like(n, d)],
        scratch_shapes=[pltpu.VMEM((heads, bq), F32), pltpu.VMEM((heads, HEAD + 8, bq), F32)],
        compiler_params=_params("arbitrary"),
        cost_estimate=_cost(2 * n * n * q.shape[1] * 2, q, k, v, wo, h, q, h),
        name="attn",
    )(q, k, v, wo, h)


def _mlp_kernel(h_ref, wg_ref, wu_ref, wd_ref, y_ref, b_s, y_s):
    c = pl.program_id(0)
    n = h_ref.shape[0]
    bt = 512

    @pl.when(c == 0)
    def _():
        b_s[...] = _normed(h_ref[...])

    for t in range(0, n, bt):
        here = slice(t, t + bt)
        gate = _dot(b_s[here, :], wg_ref[...])
        up = _dot(b_s[here, :], wu_ref[...])
        act = (gate * jax.nn.sigmoid(gate) * up).astype(BF)
        part = _dot(act, wd_ref[...])

        @pl.when(c == 0)
        def _():
            y_s[here, :] = part

        @pl.when(c > 0)
        def _():
            y_s[here, :] += part

    @pl.when(c == pl.num_programs(0) - 1)
    def _():
        y_ref[...] = (h_ref[...].astype(F32) + y_s[...].astype(BF).astype(F32)).astype(BF)


def mlp(h, wg, wu, wd, bc=512):
    n, d = h.shape
    ff = wg.shape[1]
    cols = pl.BlockSpec((d, bc), lambda c: (0, c))
    return pl.pallas_call(
        _mlp_kernel,
        grid=(ff // bc,),
        in_specs=[_whole(h.shape), cols, cols, pl.BlockSpec((bc, d), lambda c: (c, 0))],
        out_specs=_whole(h.shape),
        out_shape=_like(n, d),
        scratch_shapes=[pltpu.VMEM((n, d), BF), pltpu.VMEM((n, d), F32)],
        compiler_params=_params("arbitrary"),
        cost_estimate=_cost(6 * n * d * ff, h, h, wg, wu, wd),
        name="mlp",
    )(h, wg, wu, wd)


def _mlp_bwd_kernel(h_ref, dy_ref, wg_ref, wu_ref, wd_ref, dh_ref, dwg_ref, dwu_ref, dwd_ref, b_s, bt_s, dyt_s, db_s, act_s, dg_s, du_s):
    c = pl.program_id(0)
    n = h_ref.shape[0]
    bt = 512

    @pl.when(c == 0)
    def _():
        b = _normed(h_ref[...])
        b_s[...] = b
        bt_s[...] = b.T
        dyt_s[...] = dy_ref[...].T
        db_s[...] = jnp.zeros_like(db_s)

    for t in range(0, n, bt):
        here = slice(t, t + bt)
        gate = _dot(b_s[here, :], wg_ref[...])
        up = _dot(b_s[here, :], wu_ref[...])
        dact = _dot(dy_ref[here, :], wd_ref[...], 1, 1).astype(BF).astype(F32)
        s = jax.nn.sigmoid(gate)
        silu = gate * s
        act_s[here, :] = (silu * up).astype(BF)
        du = (dact * silu).astype(BF)
        dg = (dact * up * (s + silu * (1 - s))).astype(BF)
        du_s[here, :] = du
        dg_s[here, :] = dg
        db_s[here, :] += _dot(dg, wg_ref[...], 1, 1) + _dot(du, wu_ref[...], 1, 1)
    dwg_ref[...] = _dot(bt_s[...], dg_s[...]).astype(BF)
    dwu_ref[...] = _dot(bt_s[...], du_s[...]).astype(BF)
    dwd_ref[...] = _dot(dyt_s[...], act_s[...]).T.astype(BF)

    @pl.when(c == pl.num_programs(0) - 1)
    def _():
        dh_ref[...] = (dy_ref[...].astype(F32) + _norm_back(h_ref[...], db_s[...])).astype(BF)


def mlp_bwd(h, dy, wg, wu, wd, bc=512):
    n, d = h.shape
    ff = wg.shape[1]
    cols = pl.BlockSpec((d, bc), lambda c: (0, c))
    rows = pl.BlockSpec((bc, d), lambda c: (c, 0))
    return pl.pallas_call(
        _mlp_bwd_kernel,
        grid=(ff // bc,),
        in_specs=[_whole(h.shape), _whole(h.shape), cols, cols, rows],
        out_specs=[_whole(h.shape), cols, cols, rows],
        out_shape=[_like(n, d), _like(d, ff), _like(d, ff), _like(ff, d)],
        scratch_shapes=[pltpu.VMEM((n, d), BF), pltpu.VMEM((d, n), BF), pltpu.VMEM((d, n), BF), pltpu.VMEM((n, d), F32)]
        + [pltpu.VMEM((n, bc), BF)] * 3,
        compiler_params=_params("arbitrary"),
        cost_estimate=_cost(16 * n * d * ff, h, h, h, wg, wu, wd, wg, wu, wd),
        name="mlp_bwd",
    )(h, dy, wg, wu, wd)


def _attn_bwd_kernel(q_ref, k_ref, v_ref, o_ref, lse_ref, dh_ref, wo_ref, cos_ref, sin_ref, dq_ref, dk_ref, dv_ref, dwo_ref,
                     do_s, delta_s, dq_s, dk_s, dv_s, dwo_s, *, bk):
    bq, heads = q_ref.shape[0], q_ref.shape[1] // HEAD
    iq = pl.program_id(0)
    scale = HEAD**-0.5
    e = scale * LOG2E

    @pl.when(iq == 0)
    def _():
        dk_s[...] = jnp.zeros_like(dk_s)
        dv_s[...] = jnp.zeros_like(dv_s)
        dwo_s[...] = jnp.zeros_like(dwo_s)

    dh = dh_ref[...]
    do = _dot(dh, wo_ref[...], 1, 1).astype(BF)
    do_s[...] = do
    dwo_s[...] += _dot(o_ref[...].T, dh)
    for n in range(heads):
        own = slice(n * HEAD, (n + 1) * HEAD)
        both = do[:, own].astype(F32) * o_ref[:, own].astype(F32)
        delta_s[n : n + 1, :] = both.T.sum(axis=0, keepdims=True)
    dq_s[...] = jnp.zeros_like(dq_s)

    def block(start, at, masked):
        here = pl.ds(start, bk)
        k, v = k_ref[here, :], v_ref[here, :]
        kt = k.T
        ok = _below(bk, bq - at, 0) if masked else None
        qs = [q_ref[at:, n * HEAD : (n + 1) * HEAD] for n in range(heads)]
        dos = [do_s[at:, n * HEAD : (n + 1) * HEAD] for n in range(heads)]
        scores = [_dot(k, x, 1, 1) for x in qs]
        dps = [_dot(v, x, 1, 1) for x in dos]
        ps, dss = [], []
        for n in range(heads):
            p = jnp.exp2(scores[n] * e - lse_ref[n : n + 1, at:])
            if masked:
                p = jnp.where(ok, p, 0.0)
            ds = (p * (dps[n] - delta_s[n : n + 1, at:])).astype(BF)
            ps.append(p.astype(BF))
            dss.append(ds)
            dq_s[n, :, at:] += _dot(kt, ds)
        dv_s[here, :] += _dot(jnp.concatenate(ps, axis=1), jnp.concatenate(dos, axis=0))
        dk_s[here, :] += _dot(jnp.concatenate(dss, axis=1), jnp.concatenate(qs, axis=0))

    lax.fori_loop(0, iq * (bq // bk), lambda j, _: block(pl.multiple_of(j * bk, bk), 0, False), None)
    for at in range(0, bq, bk):
        block(pl.multiple_of(iq * bq + at, bk), at, True)
    here = pl.ds(pl.multiple_of(iq * bq, bq), bq)
    cos, sin = cos_ref[here, :], -sin_ref[here, :]
    for n in range(heads):
        dq = (dq_s[n] * scale).T.astype(BF).astype(F32)
        dq_ref[:, n * HEAD : (n + 1) * HEAD] = _turn(dq, cos, sin).astype(BF)

    @pl.when(iq == pl.num_programs(0) - 1)
    def _():
        dk = (dk_s[...] * scale).astype(BF).astype(F32)
        dk_ref[...] = _turn(dk, cos_ref[...], -sin_ref[...]).astype(BF)
        dv_ref[...] = dv_s[...].astype(BF)
        dwo_ref[...] = dwo_s[...].astype(BF)


def attn_bwd(q, k, v, o, lse, dh, wo, cos, sin, bq=512, bk=256):
    n, d = dh.shape
    heads = q.shape[1] // HEAD
    rows = lambda c: pl.BlockSpec((bq, c), lambda i: (i, 0))
    return pl.pallas_call(
        functools.partial(_attn_bwd_kernel, bk=bk),
        grid=(n // bq,),
        in_specs=[rows(q.shape[1]), _whole(k.shape), _whole(v.shape), rows(q.shape[1]), pl.BlockSpec((heads, bq), lambda i: (0, i)), rows(d),
                  _whole(wo.shape), _whole(cos.shape), _whole(sin.shape)],
        out_specs=[rows(q.shape[1]), _whole(k.shape), _whole(v.shape), _whole(wo.shape)],
        out_shape=[_like(*q.shape), _like(*k.shape), _like(*v.shape), _like(*wo.shape)],
        scratch_shapes=[pltpu.VMEM((bq, heads * HEAD), BF), pltpu.VMEM((heads, bq), F32), pltpu.VMEM((heads, HEAD, bq), F32),
                        pltpu.VMEM(k.shape, F32), pltpu.VMEM(v.shape, F32), pltpu.VMEM(wo.shape, F32)],
        compiler_params=_params("arbitrary"),
        cost_estimate=_cost(2 * n * n * q.shape[1] * 4, q, k, v, o, dh, wo, q),
        name="attn_bwd",
    )(q, k, v, o, lse, dh, wo, cos, sin)


def _qkv_bwd_kernel(h_ref, dh_ref, dq_ref, dk_ref, dv_ref, w_ref, out_ref, dw_ref, dw_s):
    i = pl.program_id(0)
    dt = jnp.concatenate([dq_ref[...], dk_ref[...], dv_ref[...]], axis=1)
    h = h_ref[...]
    da = _dot(dt, w_ref[...], 1, 1)
    out_ref[...] = (dh_ref[...].astype(F32) + _norm_back(h, da)).astype(BF)
    dw = _dot(_normed(h).T, dt)

    @pl.when(i == 0)
    def _():
        dw_s[...] = dw

    @pl.when(i > 0)
    def _():
        dw_s[...] += dw

    @pl.when(i == pl.num_programs(0) - 1)
    def _():
        dw_ref[...] = dw_s[...].astype(BF)


def qkv_bwd(h, dh, dq, dk, dv, w, bt=512):
    n, d = h.shape
    rows = lambda c: pl.BlockSpec((bt, c), lambda i: (i, 0))
    return pl.pallas_call(
        _qkv_bwd_kernel,
        grid=(n // bt,),
        in_specs=[rows(d), rows(d), rows(dq.shape[1]), rows(HEAD), rows(HEAD), _whole(w.shape)],
        out_specs=[rows(d), _whole(w.shape)],
        out_shape=[_like(n, d), _like(*w.shape)],
        scratch_shapes=[pltpu.VMEM(w.shape, F32)],
        compiler_params=_params("arbitrary"),
        cost_estimate=_cost(4 * n * d * w.shape[1], h, h, h, h, w, w),
        name="qkv_bwd",
    )(h, dh, dq, dk, dv, w)


def solution(mesh):
    def step(x, dy, wq, wk, wv, wo, wg, wu, wd):
        layers = wq.shape[0]
        d, ff = wq.shape[2], wg.shape[2]
        cos, sin = rotary(x.shape[1])
        gather = lambda w: lax.all_gather(w, "dp", axis=0, tiled=True)
        w1 = [gather(jnp.concatenate([wq[i], wk[i], wv[i]], axis=1)) for i in range(layers)]
        w2 = [gather(wo[i]) for i in range(layers)]
        w3 = [gather(jnp.concatenate([wg[i], wu[i]], axis=1)) for i in range(layers)]
        w4 = [gather(wd[i]) for i in range(layers)]
        w3 = [(t[:, :ff], t[:, ff:]) for t in w3]
        h, kept = x[0], []
        for i in range(layers):
            q, k, v = qkv(h, w1[i], cos, sin)
            o, lse, h2 = attn(q, k, v, w2[i], h)
            kept.append((h, q, k, v, o, lse, h2))
            if i + 1 < layers:
                h = mlp(h2, *w3[i], w4[i])
        dh, grads = dy[0], [None] * layers
        for i in reversed(range(layers)):
            h, q, k, v, o, lse, h2 = kept[i]
            dh2, dwg, dwu, dwd = mlp_bwd(h2, dh, *w3[i], w4[i])
            dq, dk, dv, dwo = attn_bwd(q, k, v, o, lse, dh2, w2[i], cos, sin)
            dh, dw1 = qkv_bwd(h, dh2, dq, dk, dv, w1[i])
            scatter = lambda w: lax.psum_scatter(w, "dp", scatter_dimension=0, tiled=True)
            a = scatter(jnp.concatenate([dw1, dwo, dwg, dwu], axis=1))
            b = scatter(dwd)
            at, mine = 0, []
            for wide in (d, HEAD, HEAD, d, ff, ff):
                mine.append(a[:, at : at + wide])
                at += wide
            grads[i] = [*mine, b]
        return (dh[None], *(jnp.stack([grads[i][j] for i in range(layers)]) for j in range(7)))

    states, cut = P(("rep", "dp"), None, None), P(None, "dp", None)
    return jax.shard_map(
        step,
        mesh=mesh,
        in_specs=(states, states) + (cut,) * 7,
        out_specs=(states,) + (P("rep", "dp", None),) * 7,
        check_vma=False,
    )
```

```python
import functools

import jax
import jax.numpy as jnp
import numpy as np
from jax import lax
from jax.experimental import pallas as pl
from jax.experimental.pallas import tpu as pltpu
from jax.sharding import PartitionSpec as P

HEAD = 128
THETA = 10000
EPS = 1e-6
NEG = -1e30
LOG2E = 1.4426950408889634
BF, F32 = jnp.bfloat16, jnp.float32
MIB = 2**20


def _dot(a, b, ca=1, cb=0):
    return lax.dot_general(a, b, (((ca,), (cb,)), ((), ())), preferred_element_type=F32)


def _scale(wide):
    return lax.rsqrt(jnp.mean(wide * wide, -1, keepdims=True) + EPS)


def _normed(h):
    wide = h.astype(F32)
    return (wide * _scale(wide)).astype(BF)


def _norm_back(h, da):
    wide = h.astype(F32)
    scale = _scale(wide)
    a = wide * scale
    return scale * (da - a * jnp.mean(a * da, -1, keepdims=True))


def _turn(t, cos, sin):
    return t * cos + pltpu.roll(t, t.shape[1] // 2, 1) * sin


def _whole(shape):
    return pl.BlockSpec(shape, lambda *_: (0,) * len(shape), pipeline_mode=pl.Buffered(1))


def _params(*kinds, vmem=60):
    return pltpu.CompilerParams(dimension_semantics=kinds, vmem_limit_bytes=vmem * MIB)


def _cost(flops, *arrays):
    return pl.CostEstimate(flops=flops, transcendentals=0, bytes_accessed=sum(a.size * a.dtype.itemsize for a in arrays))


def _like(*shape, dtype=BF):
    return jax.ShapeDtypeStruct(shape, dtype)


def rotary(tokens):
    half = HEAD // 2
    angle = np.arange(tokens, dtype=np.float32)[:, None] * (np.float32(THETA) ** (-np.arange(half, dtype=np.float32) / np.float32(half)))
    angle = angle.astype(np.float64)
    cos, sin = np.cos(angle), np.sin(angle)
    return np.concatenate([cos, cos], -1).astype(np.float32), np.concatenate([-sin, sin], -1).astype(np.float32)


MESH = pl.DeviceIdType.MESH
AXES = ((8, 4, 2), (4, 2, 8), (2, 8, 4))


def _flip(me, mask):
    out = me
    for bit in (1, 2, 4, 8):
        if mask & bit:
            out = out + bit * (1 - 2 * lax.rem(lax.div(me, bit), 2))
    return out


def _greet():
    me = lax.axis_index("dp")
    barrier = pltpu.get_barrier_semaphore()
    for bit in (1, 2, 4, 8):
        pl.semaphore_signal(barrier, inc=1, device_id={"dp": _flip(me, bit)}, device_id_type=MESH)
    pl.semaphore_wait(barrier, 4)


def _masks(bits):
    out = [0]
    for bit in bits:
        out += [m | bit for m in out]
    return out


class Gather:
    SENDS = 15

    @classmethod
    def scratch(cls, flows):
        return [pltpu.SemaphoreType.DMA((flows, cls.SENDS)), pltpu.SemaphoreType.DMA((flows, cls.SENDS)), pltpu.SemaphoreType.DMA((flows,))]

    def __init__(self, flows, send, recv, local):
        self.flows, self.send, self.recv, self.local = flows, send, recv, local
        self.me = lax.axis_index("dp")

    def _copy(self, f, n, mask, to):
        own, full, rows, _ = self.flows[f]
        block = _flip(self.me, mask)
        rows = slice(None) if rows is None else pl.ds(*rows)
        there = full.at[block, rows]
        return pltpu.make_async_remote_copy(
            src_ref=own.at[rows] if mask == 0 else there, dst_ref=there, send_sem=self.send.at[f, n], recv_sem=self.recv.at[f, n],
            device_id={"dp": _flip(self.me, to)}, device_id_type=MESH)

    def _here(self, f):
        own, full, rows, _ = self.flows[f]
        rows = slice(None) if rows is None else pl.ds(*rows)
        return pltpu.make_async_copy(own.at[rows], full.at[self.me, rows], self.local.at[f])

    def _list(self, f):
        order = self.flows[f][3]
        far, near, n = [], [[(7, 0, 1)]], 0
        for s in range(3):
            masks = _masks(order[:s])
            far.append([(n + i, m, order[s]) for i, m in enumerate(masks)])
            near.append([(n + 8 + i, m | order[s], 1) for i, m in enumerate(masks)])
            n += len(masks)
        return far, near

    def step(self, k):
        lists = [self._list(f) for f in range(len(self.flows))]
        if k == 0:
            for f in range(len(self.flows)):
                self._here(f).start()
        if 1 <= k <= 3:
            for f, (far, _) in enumerate(lists):
                for c in far[k - 1]:
                    self._copy(f, *c).wait_recv()
        for f, (far, near) in enumerate(lists):
            if k < 3:
                for c in far[k]:
                    self._copy(f, *c).start()
        for f, (far, near) in enumerate(lists):
            if k < 4:
                for c in near[k]:
                    self._copy(f, *c).start()
        if k == 4:
            for f, (far, near) in enumerate(lists):
                for part in near:
                    for c in part:
                        self._copy(f, *c).wait_recv()
                for part in far + near:
                    for c in part:
                        self._copy(f, *c).wait_send()
                self._here(f).wait()


ANY = pl.BlockSpec(memory_space=pl.ANY)
N_DEV = 16


def _thirds(own, full):
    rows = own.shape[0] // 3
    return [(own, full, (i * rows, rows), AXES[i]) for i in range(3)]


def _gather_kernel(own_ref, full_ref, *sems):
    g = Gather(_thirds(own_ref, full_ref), *sems)
    _greet()
    for k in range(5):
        g.step(k)


def gather(own, cid):
    full = pl.pallas_call(
        _gather_kernel,
        in_specs=[ANY],
        out_specs=ANY,
        out_shape=_like(N_DEV, *own.shape),
        scratch_shapes=Gather.scratch(3),
        compiler_params=pltpu.CompilerParams(collective_id=cid, has_side_effects=True),
        name=f"gather{cid}",
    )(own)
    return full.reshape(-1, own.shape[1])


class Scatter:
    @staticmethod
    def scratch(shapes):
        flows, out = len(shapes), []
        for r, c in shapes:
            out += [pltpu.VMEM((8, r, c), BF), pltpu.VMEM((8, r, c), BF), pltpu.VMEM((7, r, c), BF), pltpu.VMEM((7, r, c), BF)]
        return out + [pltpu.SemaphoreType.DMA((flows, 8)), pltpu.SemaphoreType.DMA((flows, 15)), pltpu.SemaphoreType.DMA((flows, 15))]

    def __init__(self, flows, refs):
        n = len(flows)
        self.flows, self.bufs = flows, [refs[4 * i : 4 * i + 4] for i in range(n)]
        self.local, self.send, self.recv = refs[4 * n :]
        self.me = lax.axis_index("dp")

    def _slots(self, f):
        a, b, c = self.flows[f][3]
        rest = [b | c, b, c, 0]
        return [a | m for m in rest] + rest

    def _block(self, f, mask):
        grad, _, rows, _ = self.flows[f]
        return grad.at[_flip(self.me, mask), slice(None) if rows is None else pl.ds(*rows)]

    def _own(self, f, n):
        return pltpu.make_async_copy(self._block(f, self._slots(f)[n]), self.bufs[f][0].at[n], self.local.at[f, n])

    def _near(self, f, n):
        return pltpu.make_async_remote_copy(
            src_ref=self._block(f, self._slots(f)[n] | 1), dst_ref=self.bufs[f][1].at[n], send_sem=self.send.at[f, n],
            recv_sem=self.recv.at[f, n], device_id={"dp": _flip(self.me, 1)}, device_id_type=MESH)

    def _far(self, f, n):
        axis = self.flows[f][3][0 if n < 4 else 1 if n < 6 else 2]
        return pltpu.make_async_remote_copy(
            src_ref=self.bufs[f][3].at[n], dst_ref=self.bufs[f][2].at[n], send_sem=self.send.at[f, 8 + n],
            recv_sem=self.recv.at[f, 8 + n], device_id={"dp": _flip(self.me, axis)}, device_id_type=MESH)

    def _sum(self, f, n):
        own, near, far, _ = self.bufs[f]
        total = own[n].astype(F32) + near[n].astype(F32)
        for i in {4: (0,), 5: (1,), 6: (2, 4), 7: (3, 5, 6)}.get(n, ()):
            total += far[i].astype(F32)
        return total.astype(BF)

    def step(self, k):
        flows = range(len(self.flows))
        if k == 0:
            for n in range(8):
                for f in flows:
                    self._near(f, n).start()
            for n in range(8):
                for f in flows:
                    self._own(f, n).start()
            return
        if k == 1:
            for f in flows:
                for n in range(8):
                    self._near(f, n).wait_recv()
                    self._own(f, n).wait()
        arrived, leave = {1: ((), range(4)), 2: (range(4), (4, 5)), 3: ((4, 5), (6,)), 4: ((6,), ())}[k]
        for f in flows:
            for n in arrived:
                self._far(f, n).wait_recv()
        for f in flows:
            for n in leave:
                self.bufs[f][3][n] = self._sum(f, n)
        for n in leave:
            for f in flows:
                self._far(f, n).start()
        if k == 4:
            for f in flows:
                _, out, rows, _ = self.flows[f]
                out[slice(None) if rows is None else pl.ds(*rows)] = self._sum(f, 7)
            for f in flows:
                for n in range(8):
                    self._near(f, n).wait_send()
                for n in range(7):
                    self._far(f, n).wait_send()


def _scatter_kernel(*refs, count):
    grads, outs, refs = refs[:count], refs[count : 2 * count], refs[2 * count :]
    s = Scatter([flow for g, o in zip(grads, outs) for flow in _cut(g, o)], refs)
    _greet()
    for k in range(5):
        s.step(k)


def _cut(grad, out):
    rows = out.shape[0] // 3
    return [(grad, out, (i * rows, rows), AXES[i]) for i in range(3)]


def _cut_shapes(*grads):
    return [(g.shape[1] // 3, g.shape[2]) for g in grads for _ in range(3)]


def _blocks(grad):
    return grad.reshape(N_DEV, -1, grad.shape[1])


def scatter(grads, cid):
    grads = [_blocks(g) for g in grads]
    return pl.pallas_call(
        functools.partial(_scatter_kernel, count=len(grads)),
        in_specs=[ANY] * len(grads),
        out_specs=[pl.BlockSpec(memory_space=pltpu.VMEM)] * len(grads),
        out_shape=[_like(*g.shape[1:]) for g in grads],
        scratch_shapes=Scatter.scratch(_cut_shapes(*grads)),
        compiler_params=pltpu.CompilerParams(collective_id=cid, has_side_effects=True, vmem_limit_bytes=40 * MIB),
        name=f"scatter{cid}",
    )(*grads)


def _below(keys, queries, first):
    gap = lax.broadcasted_iota(jnp.int32, (keys, queries), 1) - lax.broadcasted_iota(jnp.int32, (keys, queries), 0)
    return gap >= -first


def _when(step, at, run):
    pl.when(step == at)(run)


def _front_kernel(h_ref, w_ref, cos_ref, sin_ref, *refs, bq, bk, steps):
    owns, (q_ref, k_ref, v_ref, o_ref, lse_ref), fulls, (q_s, k_s, v_s, top_s, mix_s), sems = refs[:4], refs[4:9], refs[9:13], refs[13:18], refs[18:]
    i = pl.program_id(0)
    d = q_ref.shape[1]
    heads = d // HEAD
    flows = [(owns[n], fulls[n], None, AXES[n - 1]) for n in (1, 2, 3)] + _thirds(owns[0], fulls[0])
    g = Gather(flows, *sems)

    @pl.when(i == 0)
    def _():
        _greet()
        g.step(0)

    @pl.when(i == steps)
    def _():
        g.step(1)

    @pl.when(i == steps + 2)
    def _():
        g.step(2)

    @pl.when(i < steps)
    def _():
        here = pl.ds(pl.multiple_of(i * bq, bq), bq)
        a = _normed(h_ref[...])
        cos, sin = cos_ref[...], sin_ref[...]
        for n in range(0, d + 2 * HEAD, 2 * HEAD):
            t = _dot(a, w_ref[:, n : n + 2 * HEAD]).astype(BF)
            for at in (n, n + HEAD):
                own = t[:, at - n : at - n + HEAD]
                if at < d + HEAD:
                    own = _turn(own.astype(F32), cos, sin).astype(BF)
                if at < d:
                    q_ref[:, at : at + HEAD] = own
                    q_s[here, at : at + HEAD] = own
                elif at < d + HEAD:
                    k_ref[...] = own
                    k_s[here, :] = own
                else:
                    v_ref[...] = own
                    v_s[here, :] = own

    @pl.when(i >= steps)
    def _():
        iq = i - steps
        mine = pl.ds(pl.multiple_of(iq * bq, bq), bq)
        e = HEAD**-0.5 * LOG2E
        ones = jnp.ones((8, bk), BF)
        top_s[...] = jnp.full_like(top_s, NEG)
        mix_s[...] = jnp.zeros_like(mix_s)

        def block(start, at, masked):
            here = pl.ds(start, bk)
            seen_from = pl.ds(pl.multiple_of(iq * bq + at, HEAD), bq - at)
            k = k_s[here, :]
            values = jnp.concatenate([v_s[here, :].T, ones], axis=0)
            scores = [_dot(k, q_s[seen_from, n * HEAD : (n + 1) * HEAD], 1, 1) for n in range(heads)]
            ok = _below(bk, bq - at, 0) if masked else None
            weights, keeps = [], []
            for n, s in enumerate(scores):
                if masked:
                    s = jnp.where(ok, s, 2 * NEG)
                old = top_s[n : n + 1, at:]
                top = jnp.maximum(old, s.max(axis=0, keepdims=True))
                top_s[n : n + 1, at:] = top
                weights.append(jnp.exp2((s - top) * e).astype(BF))
                keeps.append(jnp.exp2((old - top) * e))
            for n, (p, keep) in enumerate(zip(weights, keeps)):
                mix_s[n, :, at:] = mix_s[n, :, at:] * keep + _dot(values, p)

        lax.fori_loop(0, iq * (bq // bk), lambda j, _: block(pl.multiple_of(j * bk, bk), 0, False), None)
        for at in range(0, bq, bk):
            block(pl.multiple_of(iq * bq + at, bk), at, True)
        for n in range(heads):
            total = mix_s[n, HEAD : HEAD + 1, :]
            o_ref[:, n * HEAD : (n + 1) * HEAD] = (mix_s[n, :HEAD, :] * (1 / total)).T.astype(BF)
            lse_ref[n : n + 1, :] = top_s[n : n + 1, :] * e + jnp.log2(total)

    @pl.when(i == 2 * steps - 1)
    def _():
        g.step(3)
        g.step(4)


def front(h, w, cos, sin, owns, cid, bq=512, bk=256):
    n, d = h.shape
    wide = w.shape[1] - 2 * HEAD
    heads, steps = wide // HEAD, n // bq
    first = lambda c: pl.BlockSpec((bq, c), lambda i: (jnp.minimum(i, steps - 1), 0))
    then = lambda c: pl.BlockSpec((bq, c), lambda i: (jnp.maximum(i - steps, 0), 0))
    out = pl.pallas_call(
        functools.partial(_front_kernel, bq=bq, bk=bk, steps=steps),
        grid=(2 * steps,),
        in_specs=[first(d), _whole(w.shape), first(HEAD), first(HEAD)] + [ANY] * 4,
        out_specs=[first(wide), first(HEAD), first(HEAD), then(wide), pl.BlockSpec((heads, bq), lambda i: (0, jnp.maximum(i - steps, 0)))] + [ANY] * 4,
        out_shape=[_like(n, wide), _like(n, HEAD), _like(n, HEAD), _like(n, wide), _like(heads, n, dtype=F32)]
        + [_like(N_DEV, *t.shape) for t in owns],
        scratch_shapes=[pltpu.VMEM((n, wide), BF), pltpu.VMEM((n, HEAD), BF), pltpu.VMEM((n, HEAD), BF),
                        pltpu.VMEM((heads, bq), F32), pltpu.VMEM((heads, HEAD + 8, bq), F32)] + Gather.scratch(6),
        compiler_params=pltpu.CompilerParams(dimension_semantics=("arbitrary",), vmem_limit_bytes=40 * MIB, collective_id=cid, has_side_effects=True),
        cost_estimate=_cost(2 * n * n * wide * 2, h, w, h, h, *[t for t in owns for _ in range(N_DEV)]),
        name=f"front{cid}",
    )(h, w, cos, sin, *owns)
    return (*out[:5], *(t.reshape(-1, t.shape[2]) for t in out[5:]))


def _after_attn(h_ref, o_ref, wo_ref, into_ref, bt=512):
    for t in range(0, h_ref.shape[0], bt):
        here = slice(t, t + bt)
        into_ref[here, :] = (h_ref[here, :].astype(F32) + _dot(o_ref[here, :], wo_ref[...]).astype(BF).astype(F32)).astype(BF)


def _mlp_kernel(x_ref, o_ref, wo_ref, wg_ref, wu_ref, wd_ref, own_ref, h_ref, y_ref, full_ref, b_s, y_s, *sems):
    c = pl.program_id(0)
    n = h_ref.shape[0]
    bt = 512
    g = Gather(_thirds(own_ref, full_ref), *sems)

    @pl.when(c == 0)
    def _():
        _greet()
        g.step(0)
        _after_attn(x_ref, o_ref, wo_ref, h_ref)
        b_s[...] = _normed(h_ref[...])

    for k in (1, 2, 3):
        _when(c, k, lambda k=k: g.step(k))

    for t in range(0, n, bt):
        here = slice(t, t + bt)
        gate = _dot(b_s[here, :], wg_ref[...])
        up = _dot(b_s[here, :], wu_ref[...])
        act = (gate * jax.nn.sigmoid(gate) * up).astype(BF)
        part = _dot(act, wd_ref[...])

        @pl.when(c == 0)
        def _():
            y_s[here, :] = part

        @pl.when(c > 0)
        def _():
            y_s[here, :] += part

    @pl.when(c == pl.num_programs(0) - 1)
    def _():
        y_ref[...] = (h_ref[...].astype(F32) + y_s[...].astype(BF).astype(F32)).astype(BF)
        g.step(4)


def mlp(x, o, wo, wg, wu, wd, own, cid, bc=512):
    n, d = x.shape
    ff = wg.shape[1]
    cols = pl.BlockSpec((d, bc), lambda c: (0, c))
    return pl.pallas_call(
        _mlp_kernel,
        grid=(ff // bc,),
        in_specs=[_whole(x.shape), _whole(o.shape), _whole(wo.shape), cols, cols, pl.BlockSpec((bc, d), lambda c: (c, 0)), ANY],
        out_specs=[_whole(x.shape), _whole(x.shape), ANY],
        out_shape=[_like(n, d), _like(n, d), _like(N_DEV, *own.shape)],
        scratch_shapes=[pltpu.VMEM((n, d), BF), pltpu.VMEM((n, d), F32)] + Gather.scratch(3),
        compiler_params=pltpu.CompilerParams(dimension_semantics=("arbitrary",), vmem_limit_bytes=60 * MIB, collective_id=cid, has_side_effects=True),
        cost_estimate=_cost(6 * n * d * ff, x, x, wg, wu, wd),
        name=f"mlp{cid}",
    )(x, o, wo, wg, wu, wd, own)


def _mlp_bwd_kernel(*refs, joins, sends):
    front, refs = refs[: 3 if joins else 1], refs[3 if joins else 1 :]
    (dy_ref, wg_ref, wu_ref, wd_ref), refs = refs[:4], refs[4:]
    grads, refs = refs[:sends], refs[sends:]
    (dh_ref, dwg_ref, dwu_ref, dwd_ref), refs = refs[:4], refs[4:]
    outs, refs = refs[:sends], refs[sends:]
    (b_s, bt_s, dyt_s, db_s, act_s, dg_s, du_s), refs = refs[:7], refs[7:]
    c = pl.program_id(0)
    if joins:
        h_ref, refs = refs[0], refs[1:]
    else:
        h_ref = front[0]
    n = h_ref.shape[0]
    bt = 512
    if joins:

        @pl.when(c == 0)
        def _():
            _after_attn(*front, h_ref)

    if sends:
        s = Scatter([flow for g, o in zip(grads, outs) for flow in _cut(g, o)], refs)

        @pl.when(c == 0)
        def _():
            _greet()
            s.step(0)

        for k in (1, 2, 3):
            _when(c, k, lambda k=k: s.step(k))

    @pl.when(c == 0)
    def _():
        b = _normed(h_ref[...])
        b_s[...] = b
        bt_s[...] = b.T
        dyt_s[...] = dy_ref[...].T
        db_s[...] = jnp.zeros_like(db_s)

    for t in range(0, n, bt):
        here = slice(t, t + bt)
        gate = _dot(b_s[here, :], wg_ref[...])
        up = _dot(b_s[here, :], wu_ref[...])
        dact = _dot(dy_ref[here, :], wd_ref[...], 1, 1).astype(BF).astype(F32)
        on = jax.nn.sigmoid(gate)
        silu = gate * on
        act_s[here, :] = (silu * up).astype(BF)
        du = (dact * silu).astype(BF)
        dg = (dact * up * (on + silu * (1 - on))).astype(BF)
        du_s[here, :] = du
        dg_s[here, :] = dg
        db_s[here, :] += _dot(dg, wg_ref[...], 1, 1) + _dot(du, wu_ref[...], 1, 1)
    dwg_ref[...] = _dot(bt_s[...], dg_s[...]).astype(BF)
    dwu_ref[...] = _dot(bt_s[...], du_s[...]).astype(BF)
    dwd_ref[...] = _dot(dyt_s[...], act_s[...]).T.astype(BF)

    @pl.when(c == pl.num_programs(0) - 1)
    def _():
        dh_ref[...] = (dy_ref[...].astype(F32) + _norm_back(h_ref[...], db_s[...])).astype(BF)
        if sends:
            s.step(4)


def mlp_bwd(state, dy, wg, wu, wd, grads=(), cid=None, bc=512):
    n, d = dy.shape
    ff = wg.shape[1]
    joins = len(state) == 3
    grads = [_blocks(g) for g in grads]
    cols = pl.BlockSpec((d, bc), lambda c: (0, c))
    rows = pl.BlockSpec((bc, d), lambda c: (c, 0))
    scratch = [pltpu.VMEM((n, d), BF), pltpu.VMEM((d, n), BF), pltpu.VMEM((d, n), BF), pltpu.VMEM((n, d), F32)] + [pltpu.VMEM((n, bc), BF)] * 3
    if joins:
        scratch += [pltpu.VMEM((n, d), BF)]
    more = {}
    if grads:
        scratch += Scatter.scratch(_cut_shapes(*grads))
        more = dict(collective_id=cid, has_side_effects=True)
    return pl.pallas_call(
        functools.partial(_mlp_bwd_kernel, joins=joins, sends=len(grads)),
        grid=(ff // bc,),
        in_specs=[_whole(t.shape) for t in (*state, dy)] + [cols, cols, rows] + [ANY] * len(grads),
        out_specs=[_whole(dy.shape), cols, cols, rows] + [_whole(g.shape[1:]) for g in grads],
        out_shape=[_like(n, d), _like(d, ff), _like(d, ff), _like(ff, d)] + [_like(*g.shape[1:]) for g in grads],
        scratch_shapes=scratch,
        compiler_params=pltpu.CompilerParams(dimension_semantics=("arbitrary",), vmem_limit_bytes=62 * MIB, **more),
        cost_estimate=_cost(16 * n * d * ff, dy, dy, dy, wg, wu, wd, wg, wu, wd),
        name=f"mlp_bwd{cid}",
    )(*state, dy, wg, wu, wd, *grads)


def _attn_bwd_kernel(q_ref, k_ref, v_ref, o_ref, lse_ref, dh_ref, wo_ref, cos_ref, sin_ref, g0_ref, g1_ref, g2_ref,
                     dq_ref, dk_ref, dv_ref, dwo_ref, r0_ref, r1_ref, r2_ref,
                     do_s, delta_s, dq_s, dk_s, dv_s, dwo_s, *refs, bk):
    bq, heads = q_ref.shape[0], q_ref.shape[1] // HEAD
    i = pl.program_id(0)
    iq = _turned_order(i)
    s = Scatter([(g0_ref, r0_ref, None, AXES[0]), (g1_ref, r1_ref, None, AXES[1]), (g2_ref, r2_ref, None, AXES[2])], refs)

    @pl.when(i == 0)
    def _():
        _greet()
        s.step(0)

    _when(i, 1, lambda: s.step(1))
    _when(i, 3, lambda: s.step(2))
    scale = HEAD**-0.5
    e = scale * LOG2E

    @pl.when(i == 0)
    def _():
        dk_s[...] = jnp.zeros_like(dk_s)
        dv_s[...] = jnp.zeros_like(dv_s)
        dwo_s[...] = jnp.zeros_like(dwo_s)

    dh = dh_ref[...]
    do = _dot(dh, wo_ref[...], 1, 1).astype(BF)
    do_s[...] = do
    dwo_s[...] += _dot(o_ref[...].T, dh)
    for n in range(heads):
        own = slice(n * HEAD, (n + 1) * HEAD)
        both = do[:, own].astype(F32) * o_ref[:, own].astype(F32)
        delta_s[n : n + 1, :] = both.T.sum(axis=0, keepdims=True)
    dq_s[...] = jnp.zeros_like(dq_s)

    def block(start, at, masked):
        here = pl.ds(start, bk)
        k, v = k_ref[here, :], v_ref[here, :]
        kt = k.T
        ok = _below(bk, bq - at, 0) if masked else None
        qs = [q_ref[at:, n * HEAD : (n + 1) * HEAD] for n in range(heads)]
        dos = [do_s[at:, n * HEAD : (n + 1) * HEAD] for n in range(heads)]
        scores = [_dot(k, x, 1, 1) for x in qs]
        dps = [_dot(v, x, 1, 1) for x in dos]
        ps, dss = [], []
        for n in range(heads):
            p = jnp.exp2(scores[n] * e - lse_ref[n : n + 1, at:])
            if masked:
                p = jnp.where(ok, p, 0.0)
            ds = (p * (dps[n] - delta_s[n : n + 1, at:])).astype(BF)
            ps.append(p.astype(BF))
            dss.append(ds)
            dq_s[n, :, at:] += _dot(kt, ds)
        dv_s[here, :] += _dot(jnp.concatenate(ps, axis=1), jnp.concatenate(dos, axis=0))
        dk_s[here, :] += _dot(jnp.concatenate(dss, axis=1), jnp.concatenate(qs, axis=0))

    lax.fori_loop(0, iq * (bq // bk), lambda j, _: block(pl.multiple_of(j * bk, bk), 0, False), None)
    _when(i, pl.num_programs(0) - 1, lambda: s.step(3))
    for at in range(0, bq, bk):
        block(pl.multiple_of(iq * bq + at, bk), at, True)
    here = pl.ds(pl.multiple_of(iq * bq, bq), bq)
    cos, sin = cos_ref[here, :], -sin_ref[here, :]
    for n in range(heads):
        dq = (dq_s[n] * scale).T.astype(BF).astype(F32)
        dq_ref[:, n * HEAD : (n + 1) * HEAD] = _turn(dq, cos, sin).astype(BF)

    @pl.when(i == pl.num_programs(0) - 1)
    def _():
        s.step(4)
        dk = (dk_s[...] * scale).astype(BF).astype(F32)
        dk_ref[...] = _turn(dk, cos_ref[...], -sin_ref[...]).astype(BF)
        dv_ref[...] = dv_s[...].astype(BF)
        dwo_ref[...] = dwo_s[...].astype(BF)


def _turned_order(i):
    return lax.rem(i + 1, 3) + 3 * lax.div(i, 3) - lax.div(i, 3) * lax.rem(i + 1, 3)


def attn_bwd(q, k, v, o, lse, dh, wo, cos, sin, grads, cid, bq=512, bk=256):
    n, d = dh.shape
    heads = q.shape[1] // HEAD
    rows = lambda c: pl.BlockSpec((bq, c), lambda i: (_turned_order(i), 0))
    grads = [_blocks(g) for g in grads]
    return pl.pallas_call(
        functools.partial(_attn_bwd_kernel, bk=bk),
        grid=(n // bq,),
        in_specs=[rows(q.shape[1]), _whole(k.shape), _whole(v.shape), rows(q.shape[1]), pl.BlockSpec((heads, bq), lambda i: (0, _turned_order(i))), rows(d),
                  _whole(wo.shape), _whole(cos.shape), _whole(sin.shape)] + [ANY] * 3,
        out_specs=[rows(q.shape[1]), _whole(k.shape), _whole(v.shape), _whole(wo.shape)] + [_whole(g.shape[1:]) for g in grads],
        out_shape=[_like(*q.shape), _like(*k.shape), _like(*v.shape), _like(*wo.shape)] + [_like(*g.shape[1:]) for g in grads],
        scratch_shapes=[pltpu.VMEM((bq, heads * HEAD), BF), pltpu.VMEM((heads, bq), F32), pltpu.VMEM((heads, HEAD, bq), F32),
                        pltpu.VMEM(k.shape, F32), pltpu.VMEM(v.shape, F32), pltpu.VMEM(wo.shape, F32)] + Scatter.scratch([g.shape[1:] for g in grads]),
        compiler_params=pltpu.CompilerParams(dimension_semantics=("arbitrary",), vmem_limit_bytes=60 * MIB, collective_id=cid, has_side_effects=True),
        cost_estimate=_cost(2 * n * n * q.shape[1] * 4, q, k, v, o, dh, wo, q),
        name=f"attn_bwd{cid}",
    )(q, k, v, o, lse, dh, wo, cos, sin, *grads)


def _qkv_bwd_kernel(h_ref, dh_ref, dq_ref, dk_ref, dv_ref, w_ref, out_ref, dw_ref, dw_s):
    i = pl.program_id(0)
    dt = jnp.concatenate([dq_ref[...], dk_ref[...], dv_ref[...]], axis=1)
    h = h_ref[...]
    da = _dot(dt, w_ref[...], 1, 1)
    out_ref[...] = (dh_ref[...].astype(F32) + _norm_back(h, da)).astype(BF)
    dw = _dot(_normed(h).T, dt)

    @pl.when(i == 0)
    def _():
        dw_s[...] = dw

    @pl.when(i > 0)
    def _():
        dw_s[...] += dw

    @pl.when(i == pl.num_programs(0) - 1)
    def _():
        dw_ref[...] = dw_s[...].astype(BF)


def qkv_bwd(h, dh, dq, dk, dv, w, bt=512):
    n, d = h.shape
    rows = lambda c: pl.BlockSpec((bt, c), lambda i: (i, 0))
    return pl.pallas_call(
        _qkv_bwd_kernel,
        grid=(n // bt,),
        in_specs=[rows(d), rows(d), rows(dq.shape[1]), rows(HEAD), rows(HEAD), _whole(w.shape)],
        out_specs=[rows(d), _whole(w.shape)],
        out_shape=[_like(n, d), _like(*w.shape)],
        scratch_shapes=[pltpu.VMEM(w.shape, F32)],
        compiler_params=_params("arbitrary"),
        cost_estimate=_cost(4 * n * d * w.shape[1], h, h, h, h, w, w),
        name="qkv_bwd",
    )(h, dh, dq, dk, dv, w)


def solution(mesh):
    def step(x, dy, wq, wk, wv, wo, wg, wu, wd):
        layers = wq.shape[0]
        d = wq.shape[2]
        cos, sin = rotary(x.shape[1])
        first = [jnp.concatenate([wq[i], wk[i], wv[i]], axis=1) for i in range(layers)]
        w1 = [gather(first[0], 0)]
        h, kept = x[0], []
        for i in range(layers):
            q, k, v, o, lse, *w = front(h, w1[i], cos, sin, (wo[i], wg[i], wu[i], wd[i]), 1 + i)
            state = (h, o, w[0])
            if i + 1 < layers:
                h2, y, more = mlp(h, o, *w, first[i + 1], 3 + i)
                w1.append(more.reshape(-1, more.shape[2]))
                state = (h2,)
            kept.append((h, q, k, v, o, lse, w, state))
            h = y
        dh, grads, late, cid = dy[0], [None] * layers, (), 10
        for i in reversed(range(layers)):
            h, q, k, v, o, lse, w, state = kept[i]
            dh2, dwg, dwu, dwd, *done = mlp_bwd(state, dh, *w[1:], late, cid)
            if late:
                grads[i + 1] += done
            dq, dk, dv, dwo, *mine = attn_bwd(q, k, v, o, lse, dh2, w[0], cos, sin, (dwg, dwu, dwd), cid + 1)
            grads[i] = mine
            dh, dw1 = qkv_bwd(h, dh2, dq, dk, dv, w1[i])
            late, cid = (dw1, dwo), cid + 2
        grads[0] += scatter(late, cid)
        outs = [(a[:, :d], a[:, d : d + HEAD], a[:, d + HEAD :], o, g, u, w) for g, u, w, a, o in grads]
        return (dh[None], *(jnp.stack([o[j] for o in outs]) for j in range(7)))

    states, cut = P(("rep", "dp"), None, None), P(None, "dp", None)
    return jax.shard_map(
        step,
        mesh=mesh,
        in_specs=(states, states) + (cut,) * 7,
        out_specs=(states,) + (P("rep", "dp", None),) * 7,
        check_vma=False,
    )
```

```python
import functools
import itertools

import jax
import jax.numpy as jnp
import numpy as np
from jax import lax
from jax.experimental import pallas as pl
from jax.experimental.pallas import tpu as pltpu
from jax.sharding import PartitionSpec as P

HEAD = 128
THETA = 10000
EPS = 1e-6
NEG = -1e30
LOG2E = 1.4426950408889634
BF, F32 = jnp.bfloat16, jnp.float32
MIB = 2**20
MOST = 62 * MIB


def _taker(refs):
    left = iter(refs)
    return lambda n=None: list(itertools.islice(left, n))


def _dot(a, b, ca=1, cb=0):
    return lax.dot_general(a, b, (((ca,), (cb,)), ((), ())), preferred_element_type=F32)


def _dot_t(a, b):
    return _dot(a, b, 1, 1)


def _scale(wide):
    return lax.rsqrt(jnp.mean(wide * wide, -1, keepdims=True) + EPS)


def _normed(h):
    wide = h.astype(F32)
    return (wide * _scale(wide)).astype(BF)


def _norm_back(h, da):
    wide = h.astype(F32)
    scale = _scale(wide)
    a = wide * scale
    return scale * (da - a * jnp.mean(a * da, -1, keepdims=True))


def _turn(t, cos, sin):
    return t * cos + pltpu.roll(t, t.shape[1] // 2, 1) * sin


def _whole(shape):
    return pl.BlockSpec(shape, lambda *_: (0,) * len(shape), pipeline_mode=pl.Buffered(1))


def _params(*kinds):
    return pltpu.CompilerParams(dimension_semantics=kinds, vmem_limit_bytes=MOST)


def _cost(flops, *arrays):
    return pl.CostEstimate(flops=flops, transcendentals=0, bytes_accessed=sum(a.size * a.dtype.itemsize for a in arrays))


def _like(*shape, dtype=BF):
    return jax.ShapeDtypeStruct(shape, dtype)


def rotary(tokens):
    half = HEAD // 2
    angle = np.arange(tokens, dtype=np.float32)[:, None] * (np.float32(THETA) ** (-np.arange(half, dtype=np.float32) / np.float32(half)))
    angle = angle.astype(np.float64)
    cos, sin = np.cos(angle), np.sin(angle)
    return np.concatenate([cos, cos], -1).astype(np.float32), np.concatenate([-sin, sin], -1).astype(np.float32)


MESH = pl.DeviceIdType.MESH
AXES = ((8, 4, 2), (4, 2, 8), (2, 8, 4))


def _flip(me, mask):
    out = me
    for bit in (1, 2, 4, 8):
        if mask & bit:
            out = out + bit * (1 - 2 * lax.rem(lax.div(me, bit), 2))
    return out


def _greet():
    me = lax.axis_index("dp")
    barrier = pltpu.get_barrier_semaphore()
    for bit in (1, 2, 4, 8):
        pl.semaphore_signal(barrier, inc=1, device_id={"dp": _flip(me, bit)}, device_id_type=MESH)
    pl.semaphore_wait(barrier, 4)


def _masks(bits):
    out = [0]
    for bit in bits:
        out += [m | bit for m in out]
    return out


class Gather:
    SENDS = 15

    @classmethod
    def scratch(cls, flows):
        return [pltpu.SemaphoreType.DMA((flows, cls.SENDS)), pltpu.SemaphoreType.DMA((flows, cls.SENDS)), pltpu.SemaphoreType.DMA((flows,))]

    def __init__(self, flows, send, recv, local):
        self.flows, self.send, self.recv, self.local = flows, send, recv, local
        self.me = lax.axis_index("dp")

    def _copy(self, f, n, mask, to):
        own, full, rows, _ = self.flows[f]
        block = _flip(self.me, mask)
        rows = slice(None) if rows is None else pl.ds(*rows)
        there = full.at[block, rows]
        own = None if mask else own
        return pltpu.make_async_remote_copy(
            src_ref=there if own is None else own.at[rows], dst_ref=there, send_sem=self.send.at[f, n], recv_sem=self.recv.at[f, n],
            device_id={"dp": _flip(self.me, to)}, device_id_type=MESH)

    def _here(self, f):
        own, full, rows, _ = self.flows[f]
        rows = slice(None) if rows is None else pl.ds(*rows)
        return pltpu.make_async_copy(own.at[rows], full.at[self.me, rows], self.local.at[f])

    def _list(self, f):
        order = self.flows[f][3]
        far, near, n = [], [[(7, 0, 1)]], 0
        for s in range(3):
            masks = _masks(order[:s])
            far.append([(n + i, m, order[s]) for i, m in enumerate(masks)])
            near.append([(n + 8 + i, m | order[s], 1) for i, m in enumerate(masks)])
            n += len(masks)
        return far, near

    def step(self, k):
        lists = [self._list(f) for f in range(len(self.flows))]
        if k == 0:
            for f, flow in enumerate(self.flows):
                if flow[0] is not None:
                    self._here(f).start()
        for f, (far, near) in enumerate(lists):
            for c in far[k - 1] if 0 < k < 4 else ():
                self._copy(f, *c).wait_recv()
            for c in far[k] if k < 3 else ():
                self._copy(f, *c).start()
        for f, (far, near) in enumerate(lists):
            for c in near[k] if k < 4 else ():
                self._copy(f, *c).start()
        if k == 4:
            for f, (far, near) in enumerate(lists):
                for part in near:
                    for c in part:
                        self._copy(f, *c).wait_recv()
                for part in far + near:
                    for c in part:
                        self._copy(f, *c).wait_send()
                if self.flows[f][0] is not None:
                    self._here(f).wait()


ANY = pl.BlockSpec(memory_space=pl.ANY)
N_DEV = 16


def _thirds(own, full):
    most = -(-full.shape[1] // 48) * 16
    return [(own, full, (i * most, min(most, full.shape[1] - i * most)), AXES[i]) for i in range(3)]


class Scatter:
    @staticmethod
    def scratch(shapes):
        flows, out = len(shapes), []
        for r, c in shapes:
            out += [pltpu.VMEM((8, r, c), BF), pltpu.VMEM((8, r, c), BF), pltpu.VMEM((7, r, c), BF), pltpu.VMEM((7, r, c), BF)]
        return out + [pltpu.SemaphoreType.DMA((flows, 8)), pltpu.SemaphoreType.DMA((flows, 15)), pltpu.SemaphoreType.DMA((flows, 15))]

    def __init__(self, flows, refs):
        n = len(flows)
        self.flows, self.bufs = flows, [refs[4 * i : 4 * i + 4] for i in range(n)]
        self.local, self.send, self.recv = refs[4 * n :]
        self.me = lax.axis_index("dp")

    def _slots(self, f):
        a, b, c = self.flows[f][3]
        rest = [b | c, b, c, 0]
        return [a | m for m in rest] + rest

    def _block(self, f, mask):
        grad, _, rows, _ = self.flows[f]
        return grad.at[_flip(self.me, mask), slice(None) if rows is None else pl.ds(*rows)]

    def _own(self, f, n):
        return pltpu.make_async_copy(self._block(f, self._slots(f)[n]), self.bufs[f][0].at[n], self.local.at[f, n])

    def _near(self, f, n):
        return pltpu.make_async_remote_copy(
            src_ref=self._block(f, self._slots(f)[n] | 1), dst_ref=self.bufs[f][1].at[n], send_sem=self.send.at[f, n],
            recv_sem=self.recv.at[f, n], device_id={"dp": _flip(self.me, 1)}, device_id_type=MESH)

    def _far(self, f, n):
        axis = self.flows[f][3][0 if n < 4 else 1 if n < 6 else 2]
        return pltpu.make_async_remote_copy(
            src_ref=self.bufs[f][3].at[n], dst_ref=self.bufs[f][2].at[n], send_sem=self.send.at[f, 8 + n],
            recv_sem=self.recv.at[f, 8 + n], device_id={"dp": _flip(self.me, axis)}, device_id_type=MESH)

    def _sum(self, f, n):
        own, near, far, _ = self.bufs[f]
        total = own[n].astype(F32) + near[n].astype(F32)
        for i in {4: (0,), 5: (1,), 6: (2, 4), 7: (3, 5, 6)}.get(n, ()):
            total += far[i].astype(F32)
        return total.astype(BF)

    def step(self, k):
        flows = range(len(self.flows))
        if k == 0:
            for n in range(8):
                for f in flows:
                    self._near(f, n).start()
            for n in range(8):
                for f in flows:
                    self._own(f, n).start()
            return
        if k == 1:
            for f in flows:
                for n in range(8):
                    self._near(f, n).wait_recv()
                    self._own(f, n).wait()
        arrived, leave = {1: ((), range(4)), 2: (range(4), (4, 5)), 3: ((4, 5), (6,)), 4: ((6,), ())}[k]
        for f in flows:
            for n in arrived:
                self._far(f, n).wait_recv()
        for f in flows:
            for n in leave:
                self.bufs[f][3][n] = self._sum(f, n)
        for n in leave:
            for f in flows:
                self._far(f, n).start()
        if k == 4:
            for f in flows:
                _, out, rows, _ = self.flows[f]
                out[slice(None) if rows is None else pl.ds(*rows)] = self._sum(f, 7)
            for f in flows:
                for n in range(8):
                    self._near(f, n).wait_send()
                for n in range(7):
                    self._far(f, n).wait_send()


def _scatter_kernel(*refs, count):
    take = _taker(refs)
    grads, outs, refs = take(count), take(count), take()
    s = Scatter([flow for g, o in zip(grads, outs) for flow in _cut(g, o)], refs)
    _greet()
    for k in range(5):
        s.step(k)


def _cut(grad, out):
    rows = out.shape[0] // 3
    return [(grad, out, (i * rows, rows), AXES[i]) for i in range(3)]


def _cut_shapes(*grads):
    return [(g.shape[1] // 3, g.shape[2]) for g in grads for _ in range(3)]


def _blocks(grad):
    return grad.reshape(N_DEV, -1, grad.shape[1])


def scatter(grads, cid):
    grads = [_blocks(g) for g in grads]
    return pl.pallas_call(
        functools.partial(_scatter_kernel, count=len(grads)),
        in_specs=[ANY] * len(grads),
        out_specs=[pl.BlockSpec(memory_space=pltpu.VMEM)] * len(grads),
        out_shape=[_like(*g.shape[1:]) for g in grads],
        scratch_shapes=Scatter.scratch(_cut_shapes(*grads)),
        compiler_params=pltpu.CompilerParams(collective_id=cid, has_side_effects=True, vmem_limit_bytes=MOST),
        name=f"scatter{cid}",
    )(*grads)


def _below(keys, queries, first):
    gap = lax.broadcasted_iota(jnp.int32, (keys, queries), 1) - lax.broadcasted_iota(jnp.int32, (keys, queries), 0)
    return gap >= -first


def _when(step, at, run):
    pl.when(step == at)(run)


def _join(pieces, into, sems):
    at, out = 0, []
    for n, piece in enumerate(pieces):
        wide = piece.shape[1]
        out.append(pltpu.make_async_copy(piece, into.at[:, pl.ds(at, wide)], sems.at[n]))
        at += wide
    return out


def _front_kernel(*refs, bq, bk, steps, layer, alone):
    take = _taker(refs)
    (h_ref, hq_ref, cos_ref, sin_ref) = take(4)
    if alone:
        (wq_ref, wk_ref, wv_ref, wo_ref) = take(4)
    else:
        (w_ref, wo_ref) = take(2)
    count = 3 if alone else 2
    owns = take(count)
    (q_ref, k_ref, v_ref, o_ref, lse_ref, h2_ref) = take(6)
    fulls = take(count)
    if alone:
        kept = take(2)
    (q_s, k_s, v_s, top_s, mix_s) = take(5)
    i = pl.program_id(0)
    d = q_ref.shape[1]
    heads = d // HEAD
    owns = [t.at[layer] for t in owns]
    if alone:
        flows = [(owns[n], fulls[n], None, AXES[n]) for n in range(3)]
    else:
        flows = [flow for n in range(2) for flow in _thirds(owns[n], fulls[n])]
    g = Gather(flows, *take(3))

    if alone:
        w_s, wo_s, join_sems, keep_sems = take(4)
        me = lax.axis_index("dp")
        small = Gather(_thirds(None, w_s) + _thirds(None, wo_s), *take(3))
        keep = [pltpu.make_async_copy(a, b, keep_sems.at[n]) for n, (a, b) in enumerate(zip((w_s, wo_s), kept))]

        @pl.when(i == 0)
        def _():
            parts = _join([t.at[layer] for t in (wq_ref, wk_ref, wv_ref)], w_s.at[me], join_sems)
            parts += _join([wo_ref.at[layer]], wo_s.at[me], keep_sems)
            for p in parts:
                p.start()
            _greet()
            for p in parts:
                p.wait()
            for n in range(3):
                small.step(n)
            g.step(0)
            for n in (3, 4):
                small.step(n)
            g.step(1)
            for p in keep:
                p.start()

        weights = lambda at, wide: w_s[:, :, at : at + wide].reshape(-1, wide)
        out_weights = lambda: wo_s[:].reshape(-1, wo_s.shape[2])
        starts, mids, last = {}, {steps + 1: 2}, (3, 4)
    else:

        @pl.when(i == 0)
        def _():
            _greet()
            g.step(0)

        weights = lambda at, wide: w_ref[:, at : at + wide]
        out_weights = lambda: wo_ref[:]
        starts, mids, last = {steps - 1: 1, steps + 2: 2}, {2 * steps - 1: 3}, (4,)

    for at, k in starts.items():
        _when(i, at, functools.partial(g.step, k))

    @pl.when(i < steps)
    def _():
        here = pl.ds(pl.multiple_of(i * bq, bq), bq)
        a = _normed(h_ref[:])
        cos, sin = cos_ref[:], sin_ref[:]
        for n in range(0, d + 2 * HEAD, 2 * HEAD):
            t = _dot(a, weights(n, 2 * HEAD)).astype(BF)
            for at in (n, n + HEAD):
                own = t[:, at - n : at - n + HEAD]
                if at < d + HEAD:
                    own = _turn(own.astype(F32), cos, sin).astype(BF)
                if at < d:
                    q_ref[:, at : at + HEAD] = own
                    q_s[here, at : at + HEAD] = own
                elif at < d + HEAD:
                    k_ref[:] = own
                    k_s[here, :] = own
                else:
                    v_ref[:] = own
                    v_s[here, :] = own

    @pl.when(i >= steps)
    def _():
        iq = i - steps
        mine = pl.ds(pl.multiple_of(iq * bq, bq), bq)
        e = HEAD**-0.5 * LOG2E
        ones = jnp.ones((8, bk), BF)
        top_s[:] = jnp.full_like(top_s, NEG)
        mix_s[:] = jnp.zeros_like(mix_s)

        def block(start, at, masked):
            here = pl.ds(start, bk)
            seen_from = pl.ds(pl.multiple_of(iq * bq + at, HEAD), bq - at)
            k = k_s[here, :]
            values = jnp.concatenate([v_s[here, :].T, ones], axis=0)
            scores = [_dot_t(k, q_s[seen_from, n * HEAD : (n + 1) * HEAD]) for n in range(heads)]
            ok = _below(bk, bq - at, 0) if masked else None
            weights, keeps = [], []
            for n, s in enumerate(scores):
                if masked:
                    s = jnp.where(ok, s, 2 * NEG)
                old = top_s[n : n + 1, at:]
                top = jnp.maximum(old, s.max(axis=0, keepdims=True))
                top_s[n : n + 1, at:] = top
                weights.append(jnp.exp2((s - top) * e).astype(BF))
                keeps.append(jnp.exp2((old - top) * e))
            for n, (p, keep) in enumerate(zip(weights, keeps)):
                mix_s[n, :, at:] = mix_s[n, :, at:] * keep + _dot(values, p)

        lax.fori_loop(0, iq * (bq // bk), lambda j, _: block(pl.multiple_of(j * bk, bk), 0, False), None)
        for at, k in mids.items():
            _when(i, at, lambda k=k: g.step(k))
        for at in range(0, bq, bk):
            block(pl.multiple_of(iq * bq + at, bk), at, True)
        outs = []
        for n in range(heads):
            total = mix_s[n, HEAD : HEAD + 1, :]
            outs.append((mix_s[n, :HEAD, :] * (1 / total)).T.astype(BF))
            lse_ref[n : n + 1, :] = top_s[n : n + 1, :] * e + jnp.log2(total)
        o = jnp.concatenate(outs, axis=1)
        o_ref[:] = o
        h2_ref[:] = (hq_ref[:].astype(F32) + _dot(o, out_weights()).astype(BF).astype(F32)).astype(BF)

    @pl.when(i == 2 * steps - 1)
    def _():
        for k in last:
            g.step(k)
        if alone:
            for p in keep:
                p.wait()


def front(h, cos, sin, weights, owns, layer, cid, bq=512, bk=512):
    n, d = h.shape
    alone = len(weights) == 4
    wide = d
    heads, steps = wide // HEAD, n // bq
    first = lambda c: pl.BlockSpec((bq, c), lambda i: (jnp.minimum(i, steps - 1), 0))
    then = lambda c: pl.BlockSpec((bq, c), lambda i: (jnp.maximum(i - steps, 0), 0))
    scratch = [pltpu.VMEM((n, wide), BF), pltpu.VMEM((n, HEAD), BF), pltpu.VMEM((n, HEAD), BF),
               pltpu.VMEM((heads, bq), F32), pltpu.VMEM((heads, HEAD + 8, bq), F32)]
    fulls = [_like(N_DEV, *t.shape[1:]) for t in owns]
    if alone:
        rows = weights[0].shape[1]
        joined = [(N_DEV, rows, wide + 2 * HEAD), (N_DEV, rows, d)]
        scratch += Gather.scratch(3) + [pltpu.VMEM(t, BF) for t in joined]
        scratch += [pltpu.SemaphoreType.DMA((3,)), pltpu.SemaphoreType.DMA((2,))] + Gather.scratch(6)
        fulls += [_like(*t) for t in joined]
        specs = [ANY] * 4
    else:
        scratch += Gather.scratch(6)
        specs = [_whole(t.shape) for t in weights]
    out = pl.pallas_call(
        functools.partial(_front_kernel, bq=bq, bk=bk, steps=steps, layer=layer, alone=alone),
        grid=(2 * steps,),
        in_specs=[first(d), then(d), first(HEAD), first(HEAD)] + specs + [ANY] * len(owns),
        out_specs=[first(wide), first(HEAD), first(HEAD), then(wide), pl.BlockSpec((heads, bq), lambda i: (0, jnp.maximum(i - steps, 0))), then(d)]
        + [ANY] * len(fulls),
        out_shape=[_like(n, wide), _like(n, HEAD), _like(n, HEAD), _like(n, wide), _like(heads, n, dtype=F32), _like(n, d)] + fulls,
        scratch_shapes=scratch,
        compiler_params=pltpu.CompilerParams(dimension_semantics=("arbitrary",), vmem_limit_bytes=MOST, collective_id=cid, has_side_effects=True),
        cost_estimate=_cost(2 * n * n * wide * 2, h, h, h, h, *[t for t in owns for _ in range(N_DEV)]),
        name=f"front{cid}",
    )(h, h, cos, sin, *weights, *owns)
    return (*out[:6], *(t.reshape(-1, t.shape[2]) for t in out[6:]))


def _mlp_kernel(h_ref, wg_ref, wu_ref, wd_ref, *refs, layer):
    take = _taker(refs)
    owns, (y_ref, *saved), fulls = take(5), take(3), take(3)
    (b_s, y_s, own_s, join_sems, *stage, save_sems), sems = take(7), take()
    c = pl.program_id(0)
    n = h_ref.shape[0]
    bt = n // 2
    owns = [t.at[layer] for t in owns]
    g = Gather([flow for own, full in zip((own_s, *owns[3:]), fulls) for flow in _thirds(own, full)], *sems)
    hooks = {(0, 1): 1, (1, 0): 2}

    wide = wg_ref.shape[1]

    def save(chunk, t):
        slot = t // bt
        cols = pl.ds(pl.multiple_of(chunk * wide, wide), wide)
        return [pltpu.make_async_copy(a.at[slot], b.at[pl.ds(t, bt), cols], save_sems.at[slot, m]) for m, (a, b) in enumerate(zip(stage, saved))]

    def free(chunk, t):
        for p in save(chunk, t):
            p.wait()

    @pl.when(c == 0)
    def _():
        parts = _join(owns[:3], own_s, join_sems)
        for p in parts:
            p.start()
        _greet()
        for p in parts:
            p.wait()
        g.step(0)
        b_s[:] = _normed(h_ref[:])

    for t in range(0, n, bt):
        for (at, sub), k in hooks.items():
            if sub == t // bt:
                _when(c, at, lambda k=k: g.step(k))
        here = slice(t, t + bt)
        gate = _dot(b_s[here, :], wg_ref[:])
        up = _dot(b_s[here, :], wu_ref[:])
        pl.when(c > 0)(functools.partial(free, c - 1, t))
        stage[0][t // bt], stage[1][t // bt] = gate, up
        for p in save(c, t):
            p.start()
        act = (gate * jax.nn.sigmoid(gate) * up).astype(BF)
        y_s[here, :] = jnp.where(c == 0, 0.0, y_s[here, :]) + _dot(act, wd_ref[:])

    @pl.when(c == pl.num_programs(0) - 1)
    def _():
        y_ref[:] = (h_ref[:].astype(F32) + y_s[:].astype(BF).astype(F32)).astype(BF)
        for k in (3, 4):
            g.step(k)
        for t in range(0, n, bt):
            free(c, t)


def mlp(h, wg, wu, wd, owns, layer, cid):
    n, d = h.shape
    ff = wg.shape[1]
    bc, bt = ff // 2, n // 2
    cols = pl.BlockSpec((d, bc), lambda c: (0, c))
    joined = (owns[0].shape[1], sum(t.shape[2] for t in owns[:3]))
    fulls = [_like(N_DEV, *joined)] + [_like(N_DEV, *t.shape[1:]) for t in owns[3:]]
    y, gate, up, *whole = pl.pallas_call(
        functools.partial(_mlp_kernel, layer=layer),
        grid=(2,),
        in_specs=[_whole(h.shape), cols, cols, pl.BlockSpec((bc, d), lambda c: (c, 0))] + [ANY] * 5,
        out_specs=[_whole(h.shape)] + [ANY] * 5,
        out_shape=[_like(n, d)] + [_like(n, ff, dtype=F32)] * 2 + fulls,
        scratch_shapes=[pltpu.VMEM((n, d), BF), pltpu.VMEM((n, d), F32), pltpu.VMEM(joined, BF), pltpu.SemaphoreType.DMA((3,))]
        + [pltpu.VMEM((2, bt, bc), F32)] * 2 + [pltpu.SemaphoreType.DMA((2, 2))] + Gather.scratch(9),
        compiler_params=pltpu.CompilerParams(dimension_semantics=("arbitrary",), vmem_limit_bytes=MOST, collective_id=cid, has_side_effects=True),
        cost_estimate=_cost(6 * n * d * ff, h, h, wg, wu, wd),
        name=f"mlp{cid}",
    )(h, wg, wu, wd, *owns)
    return (y, gate, up, *(t.reshape(-1, t.shape[2]) for t in whole))


def _mlp_bwd_kernel(*refs, sends, kept):
    take = _taker(refs)
    (h_ref, dy_ref, wg_ref, wu_ref, wd_ref) = take(5)
    grads = take(sends)
    if kept:
        saved = take(2)
    (dh_ref, dwg_ref, dwu_ref, dwd_ref) = take(4)
    outs = take(sends)
    (bt_s, dyt_s, db_s, act_s, dg_s, du_s, *stage) = take(6 + 1 + kept)
    c = pl.program_id(0)
    n = h_ref.shape[0]
    bt, group, wide = 512, n // 2, wg_ref.shape[1]
    if kept:
        load_sems = take(1)[0]
    else:
        b_s = stage[0]

    def load(chunk, t):
        slot = t // group
        cols = pl.ds(pl.multiple_of(chunk * wide, wide), wide)
        return [pltpu.make_async_copy(b.at[pl.ds(t, group), cols], a.at[slot], load_sems.at[slot, m]) for m, (a, b) in enumerate(zip(stage, saved))]

    def fetch(chunk, t):
        for p in load(chunk, t):
            p.start()

    if kept:
        _when(c, 0, lambda: fetch(0, 0))
    if sends:
        s = Scatter([flow for g, o in zip(grads, outs) for flow in _cut(g, o)], take())

        @pl.when(c == 0)
        def _():
            _greet()
            s.step(0)

        for k in (1, 2, 3):
            _when(c, k, lambda k=k: s.step(k))

    @pl.when(c == 0)
    def _():
        b = _normed(h_ref[:])
        if not kept:
            b_s[:] = b
        bt_s[:] = b.T
        dyt_s[:] = dy_ref[:].T
        db_s[:] = jnp.zeros_like(db_s)

    for t in range(0, n, bt):
        here = slice(t, t + bt)
        if not kept:
            gate = _dot(b_s[here, :], wg_ref[:])
            up = _dot(b_s[here, :], wu_ref[:])
        else:
            if t % group == 0:
                if t + group < n:
                    fetch(c, t + group)
                else:
                    pl.when(c + 1 < pl.num_programs(0))(lambda: fetch(c + 1, 0))
                for p in load(c, t):
                    p.wait()
            gate, up = (a[t // group, t % group : t % group + bt, :] for a in stage)
        dact = _dot_t(dy_ref[here, :], wd_ref[:]).astype(BF).astype(F32)
        on = jax.nn.sigmoid(gate)
        silu = gate * on
        act_s[here, :] = (silu * up).astype(BF)
        du = (dact * silu).astype(BF)
        dg = (dact * up * (on + silu * (1 - on))).astype(BF)
        du_s[here, :] = du
        dg_s[here, :] = dg
        db_s[here, :] += _dot_t(dg, wg_ref[:]) + _dot_t(du, wu_ref[:])
    dwg_ref[:] = _dot(bt_s[:], dg_s[:]).astype(BF)
    dwu_ref[:] = _dot(bt_s[:], du_s[:]).astype(BF)
    dwd_ref[:] = _dot(dyt_s[:], act_s[:]).T.astype(BF)

    @pl.when(c == pl.num_programs(0) - 1)
    def _():
        dh_ref[:] = (dy_ref[:].astype(F32) + _norm_back(h_ref[:], db_s[:])).astype(BF)
        if sends:
            s.step(4)


def mlp_bwd(h, dy, wg, wu, wd, saved, grads, cid, bc=512):
    n, d = dy.shape
    ff = wg.shape[1]
    grads = [_blocks(g) for g in grads]
    cols = pl.BlockSpec((d, bc), lambda c: (0, c))
    rows = pl.BlockSpec((bc, d), lambda c: (c, 0))
    scratch = [pltpu.VMEM((d, n), BF), pltpu.VMEM((d, n), BF), pltpu.VMEM((n, d), F32)] + [pltpu.VMEM((n, bc), BF)] * 3
    if saved:
        scratch += [pltpu.VMEM((2, n // 2, bc), F32)] * 2 + [pltpu.SemaphoreType.DMA((2, 2))]
    else:
        scratch += [pltpu.VMEM((n, d), BF)]
    more = {}
    if grads:
        scratch += Scatter.scratch(_cut_shapes(*grads))
        more = dict(collective_id=cid, has_side_effects=True)
    return pl.pallas_call(
        functools.partial(_mlp_bwd_kernel, sends=len(grads), kept=bool(saved)),
        grid=(ff // bc,),
        in_specs=[_whole(t.shape) for t in (h, dy)] + [cols, cols, rows] + [ANY] * (len(grads) + len(saved)),
        out_specs=[_whole(dy.shape), cols, cols, rows] + [_whole(g.shape[1:]) for g in grads],
        out_shape=[_like(n, d), _like(d, ff), _like(d, ff), _like(ff, d)] + [_like(*g.shape[1:]) for g in grads],
        scratch_shapes=scratch,
        compiler_params=pltpu.CompilerParams(dimension_semantics=("arbitrary",), vmem_limit_bytes=MOST, **more),
        cost_estimate=_cost(16 * n * d * ff, dy, dy, dy, wg, wu, wd, wg, wu, wd),
        name=f"mlp_bwd{cid}",
    )(h, dy, wg, wu, wd, *grads, *saved)


def _attn_bwd_kernel(q_ref, k_ref, v_ref, o_ref, lse_ref, dh_ref, wo_ref, cos_ref, sin_ref, g0_ref, g1_ref, g2_ref,
                     dq_ref, dk_ref, dv_ref, dwo_ref, r0_ref, r1_ref, r2_ref,
                     do_s, delta_s, dq_s, dk_s, dv_s, dwo_s, *refs, bk):
    bq, heads = q_ref.shape[0], q_ref.shape[1] // HEAD
    i = pl.program_id(0)
    iq = _turned_order(i)
    s = Scatter([(g0_ref, r0_ref, None, AXES[0]), (g1_ref, r1_ref, None, AXES[1]), (g2_ref, r2_ref, None, AXES[2])], refs)

    @pl.when(i == 0)
    def _():
        _greet()
        s.step(0)

    scale = HEAD**-0.5
    e = scale * LOG2E

    @pl.when(i == 0)
    def _():
        dk_s[:] = jnp.zeros_like(dk_s)
        dv_s[:] = jnp.zeros_like(dv_s)
        dwo_s[:] = jnp.zeros_like(dwo_s)

    dh = dh_ref[:]
    do = _dot_t(dh, wo_ref[:]).astype(BF)
    do_s[:] = do
    dwo_s[:] += _dot(o_ref[:].T, dh)
    for n in range(heads):
        own = slice(n * HEAD, (n + 1) * HEAD)
        both = do[:, own].astype(F32) * o_ref[:, own].astype(F32)
        delta_s[n : n + 1, :] = both.T.sum(axis=0, keepdims=True)
    dq_s[:] = jnp.zeros_like(dq_s)

    def block(start, at, masked):
        here = pl.ds(start, bk)
        k, v = k_ref[here, :], v_ref[here, :]
        kt = k.T
        ok = _below(bk, bq - at, 0) if masked else None
        qs = [q_ref[at:, n * HEAD : (n + 1) * HEAD] for n in range(heads)]
        dos = [do_s[at:, n * HEAD : (n + 1) * HEAD] for n in range(heads)]
        scores = [_dot_t(k, x) for x in qs]
        dps = [_dot_t(v, x) for x in dos]
        ps, dss = [], []
        for n in range(heads):
            p = jnp.exp2(scores[n] * e - lse_ref[n : n + 1, at:])
            if masked:
                p = jnp.where(ok, p, 0.0)
            ds = (p * (dps[n] - delta_s[n : n + 1, at:])).astype(BF)
            ps.append(p.astype(BF))
            dss.append(ds)
            dq_s[n, :, at:] += _dot(kt, ds)
        dv_s[here, :] += _dot(jnp.concatenate(ps, axis=1), jnp.concatenate(dos, axis=0))
        dk_s[here, :] += _dot(jnp.concatenate(dss, axis=1), jnp.concatenate(qs, axis=0))

    def whole(j, _):
        pl.when((i == 3) & (j == 3))(lambda: s.step(3))
        block(pl.multiple_of(j * bk, bk), 0, False)

    lax.fori_loop(0, iq * (bq // bk), whole, None)
    for at, k in {0: 1, 2: 2, 3: 4}.items():
        _when(i, at, lambda k=k: s.step(k))
    for at in range(0, bq, bk):
        block(pl.multiple_of(iq * bq + at, bk), at, True)
    here = pl.ds(pl.multiple_of(iq * bq, bq), bq)
    cos, sin = cos_ref[here, :], -sin_ref[here, :]
    for n in range(heads):
        dq = (dq_s[n] * scale).T.astype(BF).astype(F32)
        dq_ref[:, n * HEAD : (n + 1) * HEAD] = _turn(dq, cos, sin).astype(BF)

    @pl.when(i == pl.num_programs(0) - 1)
    def _():
        dk = (dk_s[:] * scale).astype(BF).astype(F32)
        dk_ref[:] = _turn(dk, cos_ref[:], -sin_ref[:]).astype(BF)
        dv_ref[:] = dv_s[:].astype(BF)
        dwo_ref[:] = dwo_s[:].astype(BF)


def _turned_order(i):
    return lax.rem(i + 1, 3) + 3 * lax.div(i, 3) - lax.div(i, 3) * lax.rem(i + 1, 3)


def attn_bwd(q, k, v, o, lse, dh, wo, cos, sin, grads, cid, bq=512, bk=256):
    n, d = dh.shape
    heads = q.shape[1] // HEAD
    rows = lambda c: pl.BlockSpec((bq, c), lambda i: (_turned_order(i), 0))
    grads = [_blocks(g) for g in grads]
    return pl.pallas_call(
        functools.partial(_attn_bwd_kernel, bk=bk),
        grid=(n // bq,),
        in_specs=[rows(q.shape[1]), _whole(k.shape), _whole(v.shape), rows(q.shape[1]), pl.BlockSpec((heads, bq), lambda i: (0, _turned_order(i))), rows(d),
                  _whole(wo.shape), _whole(cos.shape), _whole(sin.shape)] + [ANY] * 3,
        out_specs=[rows(q.shape[1]), _whole(k.shape), _whole(v.shape), _whole(wo.shape)] + [_whole(g.shape[1:]) for g in grads],
        out_shape=[_like(*q.shape), _like(*k.shape), _like(*v.shape), _like(*wo.shape)] + [_like(*g.shape[1:]) for g in grads],
        scratch_shapes=[pltpu.VMEM((bq, heads * HEAD), BF), pltpu.VMEM((heads, bq), F32), pltpu.VMEM((heads, HEAD, bq), F32),
                        pltpu.VMEM(k.shape, F32), pltpu.VMEM(v.shape, F32), pltpu.VMEM(wo.shape, F32)] + Scatter.scratch([g.shape[1:] for g in grads]),
        compiler_params=pltpu.CompilerParams(dimension_semantics=("arbitrary",), vmem_limit_bytes=MOST, collective_id=cid, has_side_effects=True),
        cost_estimate=_cost(2 * n * n * q.shape[1] * 4, q, k, v, o, dh, wo, q),
        name=f"attn_bwd{cid}",
    )(q, k, v, o, lse, dh, wo, cos, sin, *grads)


def _qkv_bwd_kernel(h_ref, dh_ref, dq_ref, dk_ref, dv_ref, w_ref, *refs, count):
    take = _taker(refs)
    parts, (out_ref, dw_ref), stacks, (dw_s,) = take(count + count), take(2), take(count), take()
    i = pl.program_id(0)
    for n, into in enumerate(stacks):

        @pl.when(i == n)
        def _():
            for layer in range(2):
                into[layer] = parts[2 * n + layer][:]

    dt = jnp.concatenate([dq_ref[:], dk_ref[:], dv_ref[:]], axis=1)
    h = h_ref[:]
    da = _dot_t(dt, w_ref[:])
    out_ref[:] = (dh_ref[:].astype(F32) + _norm_back(h, da)).astype(BF)
    dw = _dot(_normed(h).T, dt)

    @pl.when(i == 0)
    def _():
        dw_s[:] = dw

    @pl.when(i > 0)
    def _():
        dw_s[:] += dw

    @pl.when(i == pl.num_programs(0) - 1)
    def _():
        dw_ref[:] = dw_s[:].astype(BF)


def qkv_bwd(h, dh, dq, dk, dv, w, pairs=(), bt=512):
    n, d = h.shape
    rows = lambda c: pl.BlockSpec((bt, c), lambda i: (i, 0))
    parts = [t for pair in pairs for t in pair]
    return pl.pallas_call(
        functools.partial(_qkv_bwd_kernel, count=len(pairs)),
        grid=(n // bt,),
        in_specs=[rows(d), rows(d), rows(dq.shape[1]), rows(HEAD), rows(HEAD), _whole(w.shape)] + [_whole(t.shape) for t in parts],
        out_specs=[rows(d), _whole(w.shape)] + [_whole((2, *a.shape)) for a, _ in pairs],
        out_shape=[_like(n, d), _like(*w.shape)] + [_like(2, *a.shape) for a, _ in pairs],
        scratch_shapes=[pltpu.VMEM(w.shape, F32)],
        compiler_params=_params("arbitrary"),
        cost_estimate=_cost(4 * n * d * w.shape[1], h, h, h, h, w, w),
        name=f"qkv_bwd{len(pairs)}",
    )(h, dh, dq, dk, dv, w, *parts)


def solution(mesh):
    def step(x, dy, wq, wk, wv, wo, wg, wu, wd):
        d = wq.shape[2]
        cos, sin = rotary(x.shape[1])
        q, k, v, o, lse, h2, wg0, wu0, wd0, w0, wo0 = front(x[0], cos, sin, (wq, wk, wv, wo), (wg, wu, wd), 0, 1)
        h, gate, up, w1, wo1, wd1 = mlp(h2, wg0, wu0, wd0, (wq, wk, wv, wo, wd), 1, 2)
        kept = [(x[0], q, k, v, o, lse, h2)]
        q, k, v, o, lse, h2, wg1, wu1 = front(h, cos, sin, (w1, wo1), (wg, wu), 1, 3)
        kept.append((h, q, k, v, o, lse, h2))
        weights = [(w0, wo0, wg0, wu0, wd0), (w1, wo1, wg1, wu1, wd1)]
        dh, late, sums, outs = dy[0], (), [None, None], [None, None]
        for i in (1, 0):
            h, q, k, v, o, lse, h2 = kept[i]
            dh2, dwg, dwu, dwd, *outs[1] = mlp_bwd(h2, dh, *weights[i][2:], () if i else (gate, up), late, 10 + i)
            dq, dk, dv, dwo, *sums[i] = attn_bwd(q, k, v, o, lse, dh2, weights[i][1], cos, sin, (dwg, dwu, dwd), 20 + i)
            dh, dw, *stacks = qkv_bwd(h, dh2, dq, dk, dv, weights[i][0], () if i else list(zip(*sums)))
            late = (dw, dwo)
        outs[0] = scatter(late, 30)
        a, b = jnp.stack([t[0] for t in outs]), jnp.stack([t[1] for t in outs])
        return (dh[None], a[:, :, :d], a[:, :, d : d + HEAD], a[:, :, d + HEAD :], b, *stacks)

    states, cut = P(("rep", "dp"), None, None), P(None, "dp", None)
    return jax.shard_map(
        step,
        mesh=mesh,
        in_specs=(states, states) + (cut,) * 7,
        out_specs=(states,) + (P("rep", "dp", None),) * 7,
        check_vma=False,
    )
```

```python
import functools
import itertools

import jax
import jax.numpy as jnp
import numpy as np
from jax import lax
from jax.experimental import pallas as pl
from jax.experimental.pallas import tpu as pltpu
from jax.sharding import PartitionSpec as P

HEAD = 128
THETA = 10000
EPS = 1e-6
NEG = -1e30
LOG2E = 1.4426950408889634
BF, F32 = jnp.bfloat16, jnp.float32
MIB = 2**20
MOST = 62 * MIB


def _taker(refs):
    left = iter(refs)
    return lambda n=None: list(itertools.islice(left, n))


def _dot(a, b, ca=1, cb=0):
    return lax.dot_general(a, b, (((ca,), (cb,)), ((), ())), preferred_element_type=F32)


def _dot_t(a, b):
    return _dot(a, b, 1, 1)


def _scale(wide):
    return lax.rsqrt(jnp.mean(wide * wide, -1, keepdims=True) + EPS)


def _normed(h):
    wide = h.astype(F32)
    return (wide * _scale(wide)).astype(BF)


def _norm_back(h, da):
    wide = h.astype(F32)
    scale = _scale(wide)
    a = wide * scale
    return scale * (da - a * jnp.mean(a * da, -1, keepdims=True))


def _turn(t, cos, sin):
    return t * cos + pltpu.roll(t, t.shape[1] // 2, 1) * sin


def _whole(shape):
    return pl.BlockSpec(shape, lambda *_: (0,) * len(shape), pipeline_mode=pl.Buffered(1))


def _params(*kinds):
    return pltpu.CompilerParams(dimension_semantics=kinds, vmem_limit_bytes=MOST)


def _cost(flops, *arrays):
    return pl.CostEstimate(flops=flops, transcendentals=0, bytes_accessed=sum(a.size * a.dtype.itemsize for a in arrays))


def _like(*shape, dtype=BF):
    return jax.ShapeDtypeStruct(shape, dtype)


def rotary(tokens):
    half = HEAD // 2
    angle = np.arange(tokens, dtype=np.float32)[:, None] * (np.float32(THETA) ** (-np.arange(half, dtype=np.float32) / np.float32(half)))
    angle = angle.astype(np.float64)
    cos, sin = np.cos(angle), np.sin(angle)
    return np.concatenate([cos, cos], -1).astype(np.float32), np.concatenate([-sin, sin], -1).astype(np.float32)


MESH = pl.DeviceIdType.MESH
AXES = ((8, 4, 2), (4, 2, 8), (2, 8, 4))


def _flip(me, mask):
    out = me
    for bit in (1, 2, 4, 8):
        if mask & bit:
            out = out + bit * (1 - 2 * lax.rem(lax.div(me, bit), 2))
    return out


def _greet():
    me = lax.axis_index("dp")
    barrier = pltpu.get_barrier_semaphore()
    for bit in (1, 2, 4, 8):
        pl.semaphore_signal(barrier, inc=1, device_id={"dp": _flip(me, bit)}, device_id_type=MESH)
    pl.semaphore_wait(barrier, 4)


def _masks(bits):
    out = [0]
    for bit in bits:
        out += [m | bit for m in out]
    return out


class Gather:
    SENDS = 15

    @classmethod
    def scratch(cls, flows):
        return [pltpu.SemaphoreType.DMA((flows, cls.SENDS)), pltpu.SemaphoreType.DMA((flows, cls.SENDS)), pltpu.SemaphoreType.DMA((flows,))]

    def __init__(self, flows, send, recv, local):
        self.flows, self.send, self.recv, self.local = flows, send, recv, local
        self.me = lax.axis_index("dp")

    def _copy(self, f, n, mask, to):
        own, full, rows, _ = self.flows[f]
        block = _flip(self.me, mask)
        rows = slice(None) if rows is None else pl.ds(*rows)
        there = full.at[block, rows]
        own = None if mask else own
        return pltpu.make_async_remote_copy(
            src_ref=there if own is None else own.at[rows], dst_ref=there, send_sem=self.send.at[f, n], recv_sem=self.recv.at[f, n],
            device_id={"dp": _flip(self.me, to)}, device_id_type=MESH)

    def _here(self, f):
        own, full, rows, _ = self.flows[f]
        rows = slice(None) if rows is None else pl.ds(*rows)
        return pltpu.make_async_copy(own.at[rows], full.at[self.me, rows], self.local.at[f])

    def _list(self, f):
        order = self.flows[f][3]
        far, near, n = [], [[(7, 0, 1)]], 0
        for s in range(3):
            masks = _masks(order[:s])
            far.append([(n + i, m, order[s]) for i, m in enumerate(masks)])
            near.append([(n + 8 + i, m | order[s], 1) for i, m in enumerate(masks)])
            n += len(masks)
        return far, near

    def step(self, k):
        lists = [self._list(f) for f in range(len(self.flows))]
        if k == 0:
            for f, flow in enumerate(self.flows):
                if flow[0] is not None:
                    self._here(f).start()
        for f, (far, near) in enumerate(lists):
            for c in far[k - 1] if 0 < k < 4 else ():
                self._copy(f, *c).wait_recv()
            for c in far[k] if k < 3 else ():
                self._copy(f, *c).start()
        for f, (far, near) in enumerate(lists):
            for c in near[k] if k < 4 else ():
                self._copy(f, *c).start()
        if k == 4:
            for f, (far, near) in enumerate(lists):
                for part in near:
                    for c in part:
                        self._copy(f, *c).wait_recv()
                for part in far + near:
                    for c in part:
                        self._copy(f, *c).wait_send()
                if self.flows[f][0] is not None:
                    self._here(f).wait()


ANY = pl.BlockSpec(memory_space=pl.ANY)
N_DEV = 16


def _thirds(own, full):
    most = -(-full.shape[1] // 48) * 16
    return [(own, full, (i * most, min(most, full.shape[1] - i * most)), AXES[i]) for i in range(3)]


class Scatter:
    @staticmethod
    def scratch(shapes):
        flows, out = len(shapes), []
        for r, c in shapes:
            out += [pltpu.VMEM((8, r, c), BF), pltpu.VMEM((8, r, c), BF), pltpu.VMEM((7, r, c), BF), pltpu.VMEM((7, r, c), BF)]
        return out + [pltpu.SemaphoreType.DMA((flows, 8)), pltpu.SemaphoreType.DMA((flows, 15)), pltpu.SemaphoreType.DMA((flows, 15))]

    def __init__(self, flows, refs):
        n = len(flows)
        self.flows, self.bufs = flows, [refs[4 * i : 4 * i + 4] for i in range(n)]
        self.local, self.send, self.recv = refs[4 * n :]
        self.me = lax.axis_index("dp")

    def _slots(self, f):
        a, b, c = self.flows[f][3]
        rest = [b | c, b, c, 0]
        return [a | m for m in rest] + rest

    def _block(self, f, mask):
        grad, _, rows, _ = self.flows[f]
        return grad.at[_flip(self.me, mask), slice(None) if rows is None else pl.ds(*rows)]

    def _own(self, f, n):
        return pltpu.make_async_copy(self._block(f, self._slots(f)[n]), self.bufs[f][0].at[n], self.local.at[f, n])

    def _near(self, f, n):
        return pltpu.make_async_remote_copy(
            src_ref=self._block(f, self._slots(f)[n] | 1), dst_ref=self.bufs[f][1].at[n], send_sem=self.send.at[f, n],
            recv_sem=self.recv.at[f, n], device_id={"dp": _flip(self.me, 1)}, device_id_type=MESH)

    def _far(self, f, n):
        axis = self.flows[f][3][0 if n < 4 else 1 if n < 6 else 2]
        return pltpu.make_async_remote_copy(
            src_ref=self.bufs[f][3].at[n], dst_ref=self.bufs[f][2].at[n], send_sem=self.send.at[f, 8 + n],
            recv_sem=self.recv.at[f, 8 + n], device_id={"dp": _flip(self.me, axis)}, device_id_type=MESH)

    def _sum(self, f, n):
        own, near, far, _ = self.bufs[f]
        total = own[n].astype(F32) + near[n].astype(F32)
        for i in {4: (0,), 5: (1,), 6: (2, 4), 7: (3, 5, 6)}.get(n, ()):
            total += far[i].astype(F32)
        return total.astype(BF)

    def step(self, k):
        flows = range(len(self.flows))
        if k == 0:
            for n in range(8):
                for f in flows:
                    self._near(f, n).start()
            for n in range(8):
                for f in flows:
                    self._own(f, n).start()
            return
        if k == 1:
            for f in flows:
                for n in range(8):
                    self._near(f, n).wait_recv()
                    self._own(f, n).wait()
        arrived, leave = {1: ((), range(4)), 2: (range(4), (4, 5)), 3: ((4, 5), (6,)), 4: ((6,), ())}[k]
        for f in flows:
            for n in arrived:
                self._far(f, n).wait_recv()
        for f in flows:
            for n in leave:
                self.bufs[f][3][n] = self._sum(f, n)
        for n in leave:
            for f in flows:
                self._far(f, n).start()
        if k == 4:
            for f in flows:
                _, out, rows, _ = self.flows[f]
                out[slice(None) if rows is None else pl.ds(*rows)] = self._sum(f, 7)
            for f in flows:
                for n in range(8):
                    self._near(f, n).wait_send()
                for n in range(7):
                    self._far(f, n).wait_send()


def _scatter_kernel(*refs, count):
    take = _taker(refs)
    grads, outs, refs = take(count), take(count), take()
    s = Scatter([flow for g, o in zip(grads, outs) for flow in _cut(g, o)], refs)
    _greet()
    for k in range(5):
        s.step(k)


def _cut(grad, out):
    rows = out.shape[0] // 3
    return [(grad, out, (i * rows, rows), AXES[i]) for i in range(3)]


def _cut_shapes(*grads):
    return [(g.shape[1] // 3, g.shape[2]) for g in grads for _ in range(3)]


def _blocks(grad):
    return grad.reshape(N_DEV, -1, grad.shape[1])


def scatter(grads, cid):
    grads = [_blocks(g) for g in grads]
    return pl.pallas_call(
        functools.partial(_scatter_kernel, count=len(grads)),
        in_specs=[ANY] * len(grads),
        out_specs=[pl.BlockSpec(memory_space=pltpu.VMEM)] * len(grads),
        out_shape=[_like(*g.shape[1:]) for g in grads],
        scratch_shapes=Scatter.scratch(_cut_shapes(*grads)),
        compiler_params=pltpu.CompilerParams(collective_id=cid, has_side_effects=True, vmem_limit_bytes=MOST),
        name=f"scatter{cid}",
    )(*grads)


def _below(keys, queries, first):
    gap = lax.broadcasted_iota(jnp.int32, (keys, queries), 1) - lax.broadcasted_iota(jnp.int32, (keys, queries), 0)
    return gap >= -first


def _when(step, at, run):
    pl.when(step == at)(run)


def _join(pieces, into, sems):
    at, out = 0, []
    for n, piece in enumerate(pieces):
        wide = piece.shape[1]
        out.append(pltpu.make_async_copy(piece, into.at[:, pl.ds(at, wide)], sems.at[n]))
        at += wide
    return out


def _front_kernel(*refs, bq, bk, steps, layer, alone):
    take = _taker(refs)
    (h_ref, hq_ref, cos_ref, sin_ref) = take(4)
    if alone:
        (wq_ref, wk_ref, wv_ref, wo_ref) = take(4)
    else:
        (w_ref, wo_ref) = take(2)
    count = 3 if alone else 2
    owns = take(count)
    (q_ref, k_ref, v_ref, o_ref, lse_ref, h2_ref) = take(6)
    fulls = take(count)
    if alone:
        kept = take(2)
    (q_s, k_s, v_s, top_s, mix_s) = take(5)
    i = pl.program_id(0)
    d = q_ref.shape[1]
    heads = d // HEAD
    owns = [t.at[layer] for t in owns]
    if alone:
        flows = [(owns[n], fulls[n], None, AXES[n]) for n in range(3)]
    else:
        flows = [flow for n in range(2) for flow in _thirds(owns[n], fulls[n])]
    g = Gather(flows, *take(3))

    if alone:
        w_s, wo_s, join_sems, keep_sems = take(4)
        me = lax.axis_index("dp")
        now, soon = Gather(_thirds(None, w_s), *take(3)), Gather(_thirds(None, wo_s), *take(3))
        keep = [pltpu.make_async_copy(a, b, keep_sems.at[n]) for n, (a, b) in enumerate(zip((w_s, wo_s), kept))]

        @pl.when(i == 0)
        def _():
            parts = _join([t.at[layer] for t in (wq_ref, wk_ref, wv_ref)], w_s.at[me], join_sems)
            parts += _join([wo_ref.at[layer]], wo_s.at[me], keep_sems)
            for p in parts:
                p.start()
            _greet()
            for p in parts:
                p.wait()
            for n in range(3):
                now.step(n)
                soon.step(n)
            g.step(0)
            for n in (3, 4):
                now.step(n)
            keep[0].start()

        for n in (1, 2):
            _when(i, n, functools.partial(soon.step, n + 2))
        _when(i, 2, keep[1].start)

        weights = lambda at, wide: w_s[:, :, at : at + wide].reshape(-1, wide)
        out_weights = lambda: wo_s[:].reshape(-1, wo_s.shape[2])
        starts, mids = {1: 1}, {steps + 1: 2, 2 * steps - 1: 3}
    else:

        @pl.when(i == 0)
        def _():
            _greet()
            g.step(0)

        weights = lambda at, wide: w_ref[:, at : at + wide]
        out_weights = lambda: wo_ref[:]
        starts, mids = {steps - 1: 1, steps + 2: 2}, {2 * steps - 1: 3}

    for at, k in starts.items():
        _when(i, at, functools.partial(g.step, k))

    @pl.when(i < steps)
    def _():
        here = pl.ds(pl.multiple_of(i * bq, bq), bq)
        a = _normed(h_ref[:])
        cos, sin = cos_ref[:], sin_ref[:]
        for n in range(0, d + 2 * HEAD, 2 * HEAD):
            t = _dot(a, weights(n, 2 * HEAD)).astype(BF)
            for at in (n, n + HEAD):
                own = t[:, at - n : at - n + HEAD]
                if at < d + HEAD:
                    own = _turn(own.astype(F32), cos, sin).astype(BF)
                if at < d:
                    q_ref[:, at : at + HEAD] = own
                    q_s[here, at : at + HEAD] = own
                elif at < d + HEAD:
                    k_ref[:] = own
                    k_s[here, :] = own
                else:
                    v_ref[:] = own
                    v_s[here, :] = own

    @pl.when(i >= steps)
    def _():
        iq = i - steps
        mine = pl.ds(pl.multiple_of(iq * bq, bq), bq)
        e = HEAD**-0.5 * LOG2E
        ones = jnp.ones((8, bk), BF)
        top_s[:] = jnp.full_like(top_s, NEG)
        mix_s[:] = jnp.zeros_like(mix_s)

        def block(start, at, masked):
            here = pl.ds(start, bk)
            seen_from = pl.ds(pl.multiple_of(iq * bq + at, HEAD), bq - at)
            k = k_s[here, :]
            values = jnp.concatenate([v_s[here, :].T, ones], axis=0)
            scores = [_dot_t(k, q_s[seen_from, n * HEAD : (n + 1) * HEAD]) for n in range(heads)]
            ok = _below(bk, bq - at, 0) if masked else None
            weights, keeps = [], []
            for n, s in enumerate(scores):
                if masked:
                    s = jnp.where(ok, s, 2 * NEG)
                old = top_s[n : n + 1, at:]
                top = jnp.maximum(old, s.max(axis=0, keepdims=True))
                top_s[n : n + 1, at:] = top
                weights.append(jnp.exp2((s - top) * e).astype(BF))
                keeps.append(jnp.exp2((old - top) * e))
            for n, (p, keep) in enumerate(zip(weights, keeps)):
                mix_s[n, :, at:] = mix_s[n, :, at:] * keep + _dot(values, p)

        lax.fori_loop(0, iq * (bq // bk), lambda j, _: block(pl.multiple_of(j * bk, bk), 0, False), None)
        for at, k in mids.items():
            _when(i, at, lambda k=k: g.step(k))
        for at in range(0, bq, bk):
            block(pl.multiple_of(iq * bq + at, bk), at, True)
        outs = []
        for n in range(heads):
            total = mix_s[n, HEAD : HEAD + 1, :]
            outs.append((mix_s[n, :HEAD, :] * (1 / total)).T.astype(BF))
            lse_ref[n : n + 1, :] = top_s[n : n + 1, :] * e + jnp.log2(total)
        o = jnp.concatenate(outs, axis=1)
        o_ref[:] = o
        h2_ref[:] = (hq_ref[:].astype(F32) + _dot(o, out_weights()).astype(BF).astype(F32)).astype(BF)

    @pl.when(i == 2 * steps - 1)
    def _():
        g.step(4)
        if alone:
            for p in keep:
                p.wait()


def front(h, cos, sin, weights, owns, layer, cid, bq=512, bk=512):
    n, d = h.shape
    alone = len(weights) == 4
    wide = d
    heads, steps = wide // HEAD, n // bq
    first = lambda c: pl.BlockSpec((bq, c), lambda i: (jnp.minimum(i, steps - 1), 0))
    then = lambda c: pl.BlockSpec((bq, c), lambda i: (jnp.maximum(i - steps, 0), 0))
    scratch = [pltpu.VMEM((n, wide), BF), pltpu.VMEM((n, HEAD), BF), pltpu.VMEM((n, HEAD), BF),
               pltpu.VMEM((heads, bq), F32), pltpu.VMEM((heads, HEAD + 8, bq), F32)]
    fulls = [_like(N_DEV, *t.shape[1:]) for t in owns]
    if alone:
        rows = weights[0].shape[1]
        joined = [(N_DEV, rows, wide + 2 * HEAD), (N_DEV, rows, d)]
        scratch += Gather.scratch(3) + [pltpu.VMEM(t, BF) for t in joined]
        scratch += [pltpu.SemaphoreType.DMA((3,)), pltpu.SemaphoreType.DMA((2,))] + Gather.scratch(3) * 2
        fulls += [_like(*t) for t in joined]
        specs = [ANY] * 4
    else:
        scratch += Gather.scratch(6)
        specs = [_whole(t.shape) for t in weights]
    out = pl.pallas_call(
        functools.partial(_front_kernel, bq=bq, bk=bk, steps=steps, layer=layer, alone=alone),
        grid=(2 * steps,),
        in_specs=[first(d), then(d), first(HEAD), first(HEAD)] + specs + [ANY] * len(owns),
        out_specs=[first(wide), first(HEAD), first(HEAD), then(wide), pl.BlockSpec((heads, bq), lambda i: (0, jnp.maximum(i - steps, 0))), then(d)]
        + [ANY] * len(fulls),
        out_shape=[_like(n, wide), _like(n, HEAD), _like(n, HEAD), _like(n, wide), _like(heads, n, dtype=F32), _like(n, d)] + fulls,
        scratch_shapes=scratch,
        compiler_params=pltpu.CompilerParams(dimension_semantics=("arbitrary",), vmem_limit_bytes=MOST, collective_id=cid, has_side_effects=True),
        cost_estimate=_cost(2 * n * n * wide * 2, h, h, h, h, *[t for t in owns for _ in range(N_DEV)]),
        name=f"front{cid}",
    )(h, h, cos, sin, *weights, *owns)
    return (*out[:6], *(t.reshape(-1, t.shape[2]) for t in out[6:]))


def _mlp_kernel(h_ref, wg_ref, wu_ref, wd_ref, *refs, layer):
    take = _taker(refs)
    owns, (y_ref, *saved), fulls = take(5), take(3), take(3)
    (b_s, y_s, own_s, join_sems, *stage, save_sems), sems = take(7), take()
    c = pl.program_id(0)
    n = h_ref.shape[0]
    bt = n // 2
    owns = [t.at[layer] for t in owns]
    g = Gather([flow for own, full in zip((own_s, *owns[3:]), fulls) for flow in _thirds(own, full)], *sems)
    hooks = {(0, 1): 1, (1, 0): 2}

    wide = wg_ref.shape[1]

    def save(chunk, t):
        slot = t // bt
        cols = pl.ds(pl.multiple_of(chunk * wide, wide), wide)
        return [pltpu.make_async_copy(a.at[slot], b.at[pl.ds(t, bt), cols], save_sems.at[slot, m]) for m, (a, b) in enumerate(zip(stage, saved))]

    def free(chunk, t):
        for p in save(chunk, t):
            p.wait()

    @pl.when(c == 0)
    def _():
        parts = _join(owns[:3], own_s, join_sems)
        for p in parts:
            p.start()
        _greet()
        for p in parts:
            p.wait()
        g.step(0)
        b_s[:] = _normed(h_ref[:])

    for t in range(0, n, bt):
        for (at, sub), k in hooks.items():
            if sub == t // bt:
                _when(c, at, lambda k=k: g.step(k))
        here = slice(t, t + bt)
        gate = _dot(b_s[here, :], wg_ref[:])
        up = _dot(b_s[here, :], wu_ref[:])
        pl.when(c > 0)(functools.partial(free, c - 1, t))
        stage[0][t // bt], stage[1][t // bt] = gate, up
        for p in save(c, t):
            p.start()
        act = (gate * jax.nn.sigmoid(gate) * up).astype(BF)
        y_s[here, :] = jnp.where(c == 0, 0.0, y_s[here, :]) + _dot(act, wd_ref[:])

    @pl.when(c == pl.num_programs(0) - 1)
    def _():
        g.step(3)
        y_ref[:] = (h_ref[:].astype(F32) + y_s[:].astype(BF).astype(F32)).astype(BF)
        g.step(4)
        for t in range(0, n, bt):
            free(c, t)


def mlp(h, wg, wu, wd, owns, layer, cid):
    n, d = h.shape
    ff = wg.shape[1]
    bc, bt = ff // 2, n // 2
    cols = pl.BlockSpec((d, bc), lambda c: (0, c))
    joined = (owns[0].shape[1], sum(t.shape[2] for t in owns[:3]))
    fulls = [_like(N_DEV, *joined)] + [_like(N_DEV, *t.shape[1:]) for t in owns[3:]]
    y, gate, up, *whole = pl.pallas_call(
        functools.partial(_mlp_kernel, layer=layer),
        grid=(2,),
        in_specs=[_whole(h.shape), cols, cols, pl.BlockSpec((bc, d), lambda c: (c, 0))] + [ANY] * 5,
        out_specs=[_whole(h.shape)] + [ANY] * 5,
        out_shape=[_like(n, d)] + [_like(n, ff, dtype=F32)] * 2 + fulls,
        scratch_shapes=[pltpu.VMEM((n, d), BF), pltpu.VMEM((n, d), F32), pltpu.VMEM(joined, BF), pltpu.SemaphoreType.DMA((3,))]
        + [pltpu.VMEM((2, bt, bc), F32)] * 2 + [pltpu.SemaphoreType.DMA((2, 2))] + Gather.scratch(9),
        compiler_params=pltpu.CompilerParams(dimension_semantics=("arbitrary",), vmem_limit_bytes=MOST, collective_id=cid, has_side_effects=True),
        cost_estimate=_cost(6 * n * d * ff, h, h, wg, wu, wd),
        name=f"mlp{cid}",
    )(h, wg, wu, wd, *owns)
    return (y, gate, up, *(t.reshape(-1, t.shape[2]) for t in whole))


def _mlp_bwd_kernel(*refs, sends, kept):
    take = _taker(refs)
    (h_ref, dy_ref, wg_ref, wu_ref, wd_ref) = take(5)
    grads = take(sends)
    if kept:
        saved = take(2)
    (dh_ref, dwg_ref, dwu_ref, dwd_ref) = take(4)
    outs = take(sends)
    (bt_s, dyt_s, db_s, act_s, dg_s, du_s, *stage) = take(6 + 1 + kept)
    c = pl.program_id(0)
    n = h_ref.shape[0]
    bt, group, wide = 512, n // 2, wg_ref.shape[1]
    if kept:
        load_sems = take(1)[0]
    else:
        b_s = stage[0]

    def load(chunk, t):
        slot = t // group
        cols = pl.ds(pl.multiple_of(chunk * wide, wide), wide)
        return [pltpu.make_async_copy(b.at[pl.ds(t, group), cols], a.at[slot], load_sems.at[slot, m]) for m, (a, b) in enumerate(zip(stage, saved))]

    def fetch(chunk, t):
        for p in load(chunk, t):
            p.start()

    if kept:
        _when(c, 0, lambda: fetch(0, 0))
    if sends:
        s = Scatter([flow for g, o in zip(grads, outs) for flow in _cut(g, o)], take())

        @pl.when(c == 0)
        def _():
            _greet()
            s.step(0)

        for k in (1, 2, 3):
            _when(c, k, lambda k=k: s.step(k))

    @pl.when(c == 0)
    def _():
        b = _normed(h_ref[:])
        if not kept:
            b_s[:] = b
        bt_s[:] = b.T
        dyt_s[:] = dy_ref[:].T
        db_s[:] = jnp.zeros_like(db_s)

    for t in range(0, n, bt):
        here = slice(t, t + bt)
        if not kept:
            gate = _dot(b_s[here, :], wg_ref[:])
            up = _dot(b_s[here, :], wu_ref[:])
        else:
            if t % group == 0:
                if t + group < n:
                    fetch(c, t + group)
                else:
                    pl.when(c + 1 < pl.num_programs(0))(lambda: fetch(c + 1, 0))
                for p in load(c, t):
                    p.wait()
            gate, up = (a[t // group, t % group : t % group + bt, :] for a in stage)
        dact = _dot_t(dy_ref[here, :], wd_ref[:]).astype(BF).astype(F32)
        on = jax.nn.sigmoid(gate)
        silu = gate * on
        act_s[here, :] = (silu * up).astype(BF)
        du = (dact * silu).astype(BF)
        dg = (dact * up * (on + silu * (1 - on))).astype(BF)
        du_s[here, :] = du
        dg_s[here, :] = dg
        db_s[here, :] += _dot_t(dg, wg_ref[:]) + _dot_t(du, wu_ref[:])
    dwg_ref[:] = _dot(bt_s[:], dg_s[:]).astype(BF)
    dwu_ref[:] = _dot(bt_s[:], du_s[:]).astype(BF)
    dwd_ref[:] = _dot(dyt_s[:], act_s[:]).T.astype(BF)

    @pl.when(c == pl.num_programs(0) - 1)
    def _():
        dh_ref[:] = (dy_ref[:].astype(F32) + _norm_back(h_ref[:], db_s[:])).astype(BF)
        if sends:
            s.step(4)


def mlp_bwd(h, dy, wg, wu, wd, saved, grads, cid, bc=512):
    n, d = dy.shape
    ff = wg.shape[1]
    grads = [_blocks(g) for g in grads]
    cols = pl.BlockSpec((d, bc), lambda c: (0, c))
    rows = pl.BlockSpec((bc, d), lambda c: (c, 0))
    scratch = [pltpu.VMEM((d, n), BF), pltpu.VMEM((d, n), BF), pltpu.VMEM((n, d), F32)] + [pltpu.VMEM((n, bc), BF)] * 3
    if saved:
        scratch += [pltpu.VMEM((2, n // 2, bc), F32)] * 2 + [pltpu.SemaphoreType.DMA((2, 2))]
    else:
        scratch += [pltpu.VMEM((n, d), BF)]
    more = {}
    if grads:
        scratch += Scatter.scratch(_cut_shapes(*grads))
        more = dict(collective_id=cid, has_side_effects=True)
    return pl.pallas_call(
        functools.partial(_mlp_bwd_kernel, sends=len(grads), kept=bool(saved)),
        grid=(ff // bc,),
        in_specs=[_whole(t.shape) for t in (h, dy)] + [cols, cols, rows] + [ANY] * (len(grads) + len(saved)),
        out_specs=[_whole(dy.shape), cols, cols, rows] + [_whole(g.shape[1:]) for g in grads],
        out_shape=[_like(n, d), _like(d, ff), _like(d, ff), _like(ff, d)] + [_like(*g.shape[1:]) for g in grads],
        scratch_shapes=scratch,
        compiler_params=pltpu.CompilerParams(dimension_semantics=("arbitrary",), vmem_limit_bytes=MOST, **more),
        cost_estimate=_cost(16 * n * d * ff, dy, dy, dy, wg, wu, wd, wg, wu, wd),
        name=f"mlp_bwd{cid}",
    )(h, dy, wg, wu, wd, *grads, *saved)


def _attn_bwd_kernel(q_ref, k_ref, v_ref, o_ref, lse_ref, dh_ref, wo_ref, cos_ref, sin_ref, g0_ref, g1_ref, g2_ref,
                     dq_ref, dk_ref, dv_ref, dwo_ref, r0_ref, r1_ref, r2_ref,
                     do_s, delta_s, dq_s, dk_s, dv_s, dwo_s, *refs, bk):
    bq, heads = q_ref.shape[0], q_ref.shape[1] // HEAD
    i = pl.program_id(0)
    iq = _turned_order(i)
    s = Scatter([(g0_ref, r0_ref, None, AXES[0]), (g1_ref, r1_ref, None, AXES[1]), (g2_ref, r2_ref, None, AXES[2])], refs)

    @pl.when(i == 0)
    def _():
        _greet()
        s.step(0)

    _when(i, 1, functools.partial(s.step, 1))
    _when(i, 3, functools.partial(s.step, 2))

    scale = HEAD**-0.5
    e = scale * LOG2E

    @pl.when(i == 0)
    def _():
        dk_s[:] = jnp.zeros_like(dk_s)
        dv_s[:] = jnp.zeros_like(dv_s)
        dwo_s[:] = jnp.zeros_like(dwo_s)

    dh = dh_ref[:]
    do = _dot_t(dh, wo_ref[:]).astype(BF)
    do_s[:] = do
    dwo_s[:] += _dot(o_ref[:].T, dh)
    for n in range(heads):
        own = slice(n * HEAD, (n + 1) * HEAD)
        both = do[:, own].astype(F32) * o_ref[:, own].astype(F32)
        delta_s[n : n + 1, :] = both.T.sum(axis=0, keepdims=True)
    dq_s[:] = jnp.zeros_like(dq_s)

    def block(start, at, masked):
        here = pl.ds(start, bk)
        k, v = k_ref[here, :], v_ref[here, :]
        kt = k.T
        ok = _below(bk, bq - at, 0) if masked else None
        qs = [q_ref[at:, n * HEAD : (n + 1) * HEAD] for n in range(heads)]
        dos = [do_s[at:, n * HEAD : (n + 1) * HEAD] for n in range(heads)]
        scores = [_dot_t(k, x) for x in qs]
        dps = [_dot_t(v, x) for x in dos]
        ps, dss = [], []
        for n in range(heads):
            p = jnp.exp2(scores[n] * e - lse_ref[n : n + 1, at:])
            if masked:
                p = jnp.where(ok, p, 0.0)
            ds = (p * (dps[n] - delta_s[n : n + 1, at:])).astype(BF)
            ps.append(p.astype(BF))
            dss.append(ds)
            dq_s[n, :, at:] += _dot(kt, ds)
        dv_s[here, :] += _dot(jnp.concatenate(ps, axis=1), jnp.concatenate(dos, axis=0))
        dk_s[here, :] += _dot(jnp.concatenate(dss, axis=1), jnp.concatenate(qs, axis=0))

    def whole(j, _):
        pl.when((i == 3) & (j == 5))(lambda: s.step(3))
        block(pl.multiple_of(j * bk, bk), 0, False)

    lax.fori_loop(0, iq * (bq // bk), whole, None)
    for at in range(0, bq, bk):
        block(pl.multiple_of(iq * bq + at, bk), at, True)
    here = pl.ds(pl.multiple_of(iq * bq, bq), bq)
    cos, sin = cos_ref[here, :], -sin_ref[here, :]
    for n in range(heads):
        dq = (dq_s[n] * scale).T.astype(BF).astype(F32)
        dq_ref[:, n * HEAD : (n + 1) * HEAD] = _turn(dq, cos, sin).astype(BF)

    @pl.when(i == pl.num_programs(0) - 1)
    def _():
        dk = (dk_s[:] * scale).astype(BF).astype(F32)
        dk_ref[:] = _turn(dk, cos_ref[:], -sin_ref[:]).astype(BF)
        dv_ref[:] = dv_s[:].astype(BF)
        dwo_ref[:] = dwo_s[:].astype(BF)
        s.step(4)


def _turned_order(i):
    return lax.rem(i + 1, 3) + 3 * lax.div(i, 3) - lax.div(i, 3) * lax.rem(i + 1, 3)


def attn_bwd(q, k, v, o, lse, dh, wo, cos, sin, grads, cid, bq=512, bk=256):
    n, d = dh.shape
    heads = q.shape[1] // HEAD
    rows = lambda c: pl.BlockSpec((bq, c), lambda i: (_turned_order(i), 0))
    grads = [_blocks(g) for g in grads]
    return pl.pallas_call(
        functools.partial(_attn_bwd_kernel, bk=bk),
        grid=(n // bq,),
        in_specs=[rows(q.shape[1]), _whole(k.shape), _whole(v.shape), rows(q.shape[1]), pl.BlockSpec((heads, bq), lambda i: (0, _turned_order(i))), rows(d),
                  _whole(wo.shape), _whole(cos.shape), _whole(sin.shape)] + [ANY] * 3,
        out_specs=[rows(q.shape[1]), _whole(k.shape), _whole(v.shape), _whole(wo.shape)] + [_whole(g.shape[1:]) for g in grads],
        out_shape=[_like(*q.shape), _like(*k.shape), _like(*v.shape), _like(*wo.shape)] + [_like(*g.shape[1:]) for g in grads],
        scratch_shapes=[pltpu.VMEM((bq, heads * HEAD), BF), pltpu.VMEM((heads, bq), F32), pltpu.VMEM((heads, HEAD, bq), F32),
                        pltpu.VMEM(k.shape, F32), pltpu.VMEM(v.shape, F32), pltpu.VMEM(wo.shape, F32)] + Scatter.scratch([g.shape[1:] for g in grads]),
        compiler_params=pltpu.CompilerParams(dimension_semantics=("arbitrary",), vmem_limit_bytes=MOST, collective_id=cid, has_side_effects=True),
        cost_estimate=_cost(2 * n * n * q.shape[1] * 4, q, k, v, o, dh, wo, q),
        name=f"attn_bwd{cid}",
    )(q, k, v, o, lse, dh, wo, cos, sin, *grads)


def _qkv_bwd_kernel(h_ref, dh_ref, dq_ref, dk_ref, dv_ref, w_ref, *refs, count):
    take = _taker(refs)
    parts, (out_ref, dw_ref), stacks, (dw_s,) = take(count + count), take(2), take(count), take()
    i = pl.program_id(0)
    for n, into in enumerate(stacks):

        @pl.when(i == n)
        def _():
            for layer in range(2):
                into[layer] = parts[2 * n + layer][:]

    dt = jnp.concatenate([dq_ref[:], dk_ref[:], dv_ref[:]], axis=1)
    h = h_ref[:]
    da = _dot_t(dt, w_ref[:])
    out_ref[:] = (dh_ref[:].astype(F32) + _norm_back(h, da)).astype(BF)
    dw = _dot(_normed(h).T, dt)

    @pl.when(i == 0)
    def _():
        dw_s[:] = dw

    @pl.when(i > 0)
    def _():
        dw_s[:] += dw

    @pl.when(i == pl.num_programs(0) - 1)
    def _():
        dw_ref[:] = dw_s[:].astype(BF)


def qkv_bwd(h, dh, dq, dk, dv, w, pairs=(), bt=512):
    n, d = h.shape
    rows = lambda c: pl.BlockSpec((bt, c), lambda i: (i, 0))
    parts = [t for pair in pairs for t in pair]
    return pl.pallas_call(
        functools.partial(_qkv_bwd_kernel, count=len(pairs)),
        grid=(n // bt,),
        in_specs=[rows(d), rows(d), rows(dq.shape[1]), rows(HEAD), rows(HEAD), _whole(w.shape)] + [_whole(t.shape) for t in parts],
        out_specs=[rows(d), _whole(w.shape)] + [_whole((2, *a.shape)) for a, _ in pairs],
        out_shape=[_like(n, d), _like(*w.shape)] + [_like(2, *a.shape) for a, _ in pairs],
        scratch_shapes=[pltpu.VMEM(w.shape, F32)],
        compiler_params=_params("arbitrary"),
        cost_estimate=_cost(4 * n * d * w.shape[1], h, h, h, h, w, w),
        name=f"qkv_bwd{len(pairs)}",
    )(h, dh, dq, dk, dv, w, *parts)


def solution(mesh):
    def step(x, dy, wq, wk, wv, wo, wg, wu, wd):
        d = wq.shape[2]
        cos, sin = rotary(x.shape[1])
        q, k, v, o, lse, h2, wg0, wu0, wd0, w0, wo0 = front(x[0], cos, sin, (wq, wk, wv, wo), (wg, wu, wd), 0, 1)
        h, gate, up, w1, wo1, wd1 = mlp(h2, wg0, wu0, wd0, (wq, wk, wv, wo, wd), 1, 2)
        kept = [(x[0], q, k, v, o, lse, h2)]
        q, k, v, o, lse, h2, wg1, wu1 = front(h, cos, sin, (w1, wo1), (wg, wu), 1, 3)
        kept.append((h, q, k, v, o, lse, h2))
        weights = [(w0, wo0, wg0, wu0, wd0), (w1, wo1, wg1, wu1, wd1)]
        dh, late, sums, outs = dy[0], (), [None, None], [None, None]
        for i in (1, 0):
            h, q, k, v, o, lse, h2 = kept[i]
            dh2, dwg, dwu, dwd, *outs[1] = mlp_bwd(h2, dh, *weights[i][2:], () if i else (gate, up), late, 10 + i)
            dq, dk, dv, dwo, *sums[i] = attn_bwd(q, k, v, o, lse, dh2, weights[i][1], cos, sin, (dwg, dwu, dwd), 20 + i)
            dh, dw, *stacks = qkv_bwd(h, dh2, dq, dk, dv, weights[i][0], () if i else list(zip(*sums)))
            late = (dw, dwo)
        outs[0] = scatter(late, 30)
        a, b = jnp.stack([t[0] for t in outs]), jnp.stack([t[1] for t in outs])
        return (dh[None], a[:, :, :d], a[:, :, d : d + HEAD], a[:, :, d + HEAD :], b, *stacks)

    states, cut = P(("rep", "dp"), None, None), P(None, "dp", None)
    return jax.shard_map(
        step,
        mesh=mesh,
        in_specs=(states, states) + (cut,) * 7,
        out_specs=(states,) + (P("rep", "dp", None),) * 7,
        check_vma=False,
    )
```
